32 devices in a mesh: row: 8 (over y, x, core), col: 4 (over z).
Axes of the slice: x: 2, y: 2, z: 4, core: 2. Of those that a mesh axis runs over, the one named last changes fastest.
Arguments:
- species: bfloat16 [3, 512, 512, 256], P(None, 'row', 'col'), may hold values from -6 to 6
- flow_field: bfloat16 [3, 512, 512, 256], P(None, 'row', 'col'), may hold values from -6 to 6
- x_operators: bfloat16 [2, 512, 512], replicated, may hold values from -8 to 8
- y_operators: bfloat16 [2, 512, 512], replicated, may hold values from -8 to 8
Outputs:
- species_derivatives: bfloat16 [3, 2, 512, 512, 256], P(None, None, 'row', 'col')
- flow_derivatives: bfloat16 [3, 2, 512, 512, 256], P(None, None, 'row', 'col')
The draws below stay inside these ranges and needn't reach their ends.
All inputs are finite; a program needn't handle non-finite values.
Results may differ from the reference program's by a relative error of at most 0.001.
Values may be sent and summed in bfloat16 or wider, within the bound.
A program may use at most 256 MiB of HBM per device.

```python
import jax
import jax.numpy as jnp
from jax import lax

NX = 512
NY = 512
NZ = 256


def operator_pair(key, length):
    index = jnp.arange(length)
    offset = (index[None, :] - index[:, None]) % length

    def band(shift):
        return (offset == shift).astype(jnp.float32)
    ident = band(0)
    plus_one = band(1)
    minus_one = band(length - 1)
    plus_two = band(2)
    minus_two = band(length - 2)
    first_lhs = ident + (plus_one + minus_one) / 3.0
    first_rhs = 14.0 / 9.0 * (plus_one - minus_one) / 2.0 + 1.0 / 9.0 * (plus_two - minus_two) / 4.0
    second_lhs = ident + 2.0 / 11.0 * (plus_one + minus_one)
    second_rhs = 12.0 / 11.0 * (plus_one + minus_one - 2.0 * ident) + 3.0 / 11.0 * (plus_two + minus_two - 2.0 * ident) / 4.0
    first = jnp.linalg.solve(first_lhs, first_rhs)
    second = jnp.linalg.solve(second_lhs, second_rhs)
    keys = jax.random.split(key, 2)
    spacing = jnp.exp(jax.random.uniform(keys[0], (length,), jnp.float32, jnp.log(0.6), jnp.log(1.6)))
    extra = 0.5 * jax.random.normal(keys[1], (2, length, length), jnp.float32) / jnp.sqrt(length * 1.0)
    first = spacing[:, None] * first
    second = 0.25 * (spacing * spacing)[:, None] * second
    whole = jnp.stack([first, second]) + extra
    return jnp.clip(whole, -8.0, 8.0).astype(jnp.bfloat16)


def draw_x_operators(key, part):
    return operator_pair(jax.random.fold_in(key, 11), NX)


def draw_y_operators(key, part):
    return operator_pair(jax.random.fold_in(key, 23), NY)


def shard_levels(own_key, shape, shards, least, top_value):
    gain = 1.0
    for axis_at, shards_of in shards:
        draws = jax.random.uniform(jax.random.fold_in(jax.random.fold_in(own_key, 6), axis_at), (shards_of,), jnp.float32, least / len(shards), top_value / len(shards))
        gain = gain * jnp.repeat(jnp.exp(draws), shape[axis_at] // shards_of).reshape((-1,) + (1,) * (len(shape) - 1 - axis_at))
    return gain


def centred(own_key, dims, scale, limit, shards=(), dtype=jnp.bfloat16):
    array = scale * jax.random.normal(own_key, dims, jnp.float32)
    if shards:
        array = array * shard_levels(own_key, dims, shards, -0.22, 0.18)
    return jnp.clip(array, -limit, limit).astype(dtype)


def setup_inputs(seed: int = 0) -> dict:
    key_of = jax.random.split(jax.random.key(seed), 5)
    return {
        "species": centred(key_of[0], (3, NX, NY, NZ), 1.0, 6.0, ((1, 8), (2, 4))),
        "flow_field": centred(key_of[1], (3, NX, NY, NZ), 1.0, 6.0, ((1, 8), (2, 4))),
        "x_operators": draw_x_operators(jax.random.fold_in(key_of[4], 71), 0),
        "y_operators": draw_y_operators(jax.random.fold_in(key_of[4], 71), 0),
    }


def along_first(operators, field):
    ops = operators.astype(jnp.float32)
    values = field.astype(jnp.float32)
    first = jnp.einsum('ij,jyz->iyz', ops[0], values, precision=lax.Precision.HIGHEST)
    second = jnp.einsum('ij,jyz->iyz', ops[1], values, precision=lax.Precision.HIGHEST)
    return jnp.stack([first.astype(jnp.bfloat16), second.astype(jnp.bfloat16)])

def along_second(operators, field):
    ops = operators.astype(jnp.float32)
    values = field.astype(jnp.float32)
    first = jnp.einsum('ij,xjz->xiz', ops[0], values, precision=lax.Precision.HIGHEST)
    second = jnp.einsum('ij,xjz->xiz', ops[1], values, precision=lax.Precision.HIGHEST)
    return jnp.stack([first.astype(jnp.bfloat16), second.astype(jnp.bfloat16)])

def reference(species, flow_field, x_operators, y_operators):
    species_derivatives = lax.map(lambda field: along_first(x_operators, field), species)
    flow_derivatives = lax.map(lambda field: along_second(y_operators, field), flow_field)
    return (species_derivatives, flow_derivatives)
```

```python
import functools

import jax
import jax.numpy as jnp
from jax import lax
from jax.experimental import pallas as pl
from jax.experimental.pallas import tpu as pltpu
from jax.sharding import PartitionSpec as P


FLOW_SPLITS = 4
AHEAD = 3
BEHIND = 3
LAG = 1
VMEM = 56 * 1024 * 1024


def params():
    return pltpu.CompilerParams(vmem_limit_bytes=VMEM)


def cost(flops, moved):
    return pl.CostEstimate(flops=flops, bytes_accessed=moved, transcendentals=0)


TOKEN = jax.ShapeDtypeStruct((8, 128), jnp.float32)
TOKEN_SPEC = pl.BlockSpec((8, 128), lambda g: (0, 0))
ANY_SPEC = pl.BlockSpec(memory_space=pl.ANY)


def flow_kernel(count, ahead, w_ref, *refs):
    sources, (own_ref, served_ref) = refs[:count], refs[-2 - ahead :][:2]
    width = own_ref.shape[3]
    if ahead:
        refs[-1][...] = refs[count][0]

    @pl.loop(0, own_ref.shape[2])
    def _(x):
        lines = jnp.concatenate(
            [s[0, x] if len(s.shape) == 4 else s[x] for s in sources], axis=0
        )
        out = jnp.dot(w_ref[...], lines, preferred_element_type=jnp.float32)
        out = out.astype(jnp.bfloat16)
        for d in range(2):
            own_ref[0, d, x] = out[d * width : (d + 1) * width]
            served_ref[d, x] = out[(2 + d) * width : (3 + d) * width]


def flow_compute(weights, flow, received, s, start, rows, ahead, tokens):
    _, _, width, depth = flow.shape
    tile = min(rows, 4)
    block = pl.BlockSpec((tile, width, depth), lambda g: (g, 0, 0))

    def piece_of(s, start):
        return pl.BlockSpec((1, tile, width, depth), lambda g: (s, start // tile + g, 0, 0))

    n = weights.shape[1]
    later = [] if ahead is None else [ahead]
    return pl.pallas_call(
        functools.partial(flow_kernel, 1 + len(received), len(later)),
        grid=(rows // tile,),
        in_specs=[pl.BlockSpec(weights.shape, lambda g: (0, 0)), piece_of(s, start)]
        + [block] * len(received)
        + [piece_of(*at) for at in later]
        + [ANY_SPEC] * len(tokens),
        out_specs=[
            pl.BlockSpec((1, 2, tile, width, depth), lambda g: (0, 0, g, 0, 0)),
            pl.BlockSpec((2, tile, width, depth), lambda g: (0, g, 0, 0)),
        ]
        + [block] * len(later),
        out_shape=[
            jax.ShapeDtypeStruct((1, 2, rows, width, depth), jnp.bfloat16),
            jax.ShapeDtypeStruct((2, rows, width, depth), jnp.bfloat16),
        ]
        + [jax.ShapeDtypeStruct((rows, width, depth), jnp.bfloat16)] * len(later),
        compiler_params=params(),
        cost_estimate=cost(8 * rows * width * n * depth, 2 * rows * depth * (n + 4 * width)),
        name="flow_compute",
    )(weights, flow, *received, *[flow for _ in later], *tokens)


def pick_kernel(count, quarter, own_ref, got_ref, *refs):
    out_ref, token_ref = refs[-2:]
    me = lax.axis_index("col")
    inner = jnp.logical_and(me >= quarter, me < count - quarter)
    token_ref[...] = jnp.zeros_like(token_ref)

    @pl.when(inner)
    def _():
        out_ref[...] = own_ref[...]

    @pl.when(jnp.logical_not(inner))
    def _():
        out_ref[0] = got_ref[...]


def flow_pick(shape, own, got, whole, s, start, rows, count):
    tile = min(rows, 4)
    width, depth = shape[3:]
    operands = (own, got) + (() if whole is None else (whole,))
    return pl.pallas_call(
        functools.partial(pick_kernel, count, count // 4),
        grid=(rows // tile,),
        in_specs=[
            pl.BlockSpec((1, 2, tile, width, depth), lambda g: (0, 0, g, 0, 0)),
            pl.BlockSpec((2, tile, width, depth), lambda g: (0, g, 0, 0)),
        ]
        + [ANY_SPEC] * (len(operands) - 2),
        out_specs=[
            pl.BlockSpec(
                (1, 2, tile, width, depth), lambda g: (s, 0, start // tile + g, 0, 0)
            ),
            TOKEN_SPEC,
        ],
        out_shape=[jax.ShapeDtypeStruct(shape, jnp.bfloat16), TOKEN],
        input_output_aliases={2: 0} if whole is not None else {},
        compiler_params=params(),
        cost_estimate=cost(0, 12 * rows * width * depth),
        name="flow_pick",
    )(*operands)


def turn_kernel(in_ref, out_ref, scratch):
    _, width, tile, depth = in_ref.shape
    for h in range(depth // 128):
        part = in_ref[0, :, :, h * 128 : (h + 1) * 128].astype(jnp.float32)
        scratch[h] = part.reshape(width * tile, 128)
    for y in range(tile):
        for h in range(depth // 128):
            out_ref[y, :, h * 128 : (h + 1) * 128] = scratch[
                h, pl.ds(y, width, stride=tile), :
            ].astype(jnp.bfloat16)


def turn(species, s):
    _, width, rows, depth = species.shape
    tile = 16
    return pl.pallas_call(
        turn_kernel,
        grid=(rows // tile,),
        in_specs=[pl.BlockSpec((1, width, tile, depth), lambda g: (s, 0, g, 0))],
        out_specs=pl.BlockSpec((tile, width, depth), lambda g: (g, 0, 0)),
        out_shape=jax.ShapeDtypeStruct((rows, width, depth), jnp.bfloat16),
        scratch_shapes=[pltpu.VMEM((depth // 128, width * tile, 128), jnp.float32)],
        compiler_params=params(),
        cost_estimate=cost(0, 4 * rows * width * depth),
        name="turn",
    )(species)


def species_kernel(w_ref, lines_ref, *refs):
    out_ref, token_ref, scratch = refs[-3:]
    _, _, width, tile, depth = out_ref.shape
    token_ref[...] = jnp.zeros_like(token_ref)

    for y in range(tile):
        lines = jnp.concatenate([lines_ref[k, y] for k in range(lines_ref.shape[0])], axis=0)
        out = jnp.dot(w_ref[...], lines, preferred_element_type=jnp.float32)
        for h in range(depth // 128):
            scratch[h, pl.ds(y, 2 * width, stride=tile), :] = out[:, h * 128 : (h + 1) * 128]
    for h in range(depth // 128):
        for d in range(2):
            part = scratch[h, d * width * tile : (d + 1) * width * tile, :]
            out_ref[0, d, :, :, h * 128 : (h + 1) * 128] = part.reshape(
                width, tile, 128
            ).astype(jnp.bfloat16)


def species_compute(shape, weights, lines, whole, s, start, tokens):
    _, _, width, _, depth = shape
    count, rows = lines.shape[:2]
    tile = 16
    operands = (weights, lines) + (() if whole is None else (whole,)) + tuple(tokens)
    n = weights.shape[1]
    return pl.pallas_call(
        species_kernel,
        grid=(rows // tile,),
        in_specs=[
            pl.BlockSpec(weights.shape, lambda g: (0, 0)),
            pl.BlockSpec((count, tile, width, depth), lambda g: (0, g, 0, 0)),
        ]
        + [ANY_SPEC] * (len(operands) - 2),
        out_specs=[
            pl.BlockSpec(
                (1, 2, width, tile, depth), lambda g: (s, 0, 0, start // tile + g, 0)
            ),
            TOKEN_SPEC,
        ],
        out_shape=[jax.ShapeDtypeStruct(shape, jnp.bfloat16), TOKEN],
        scratch_shapes=[pltpu.VMEM((depth // 128, 2 * width * tile, 128), jnp.float32)],
        input_output_aliases={2: 0} if whole is not None else {},
        compiler_params=params(),
        cost_estimate=cost(4 * rows * width * n * depth, 2 * rows * depth * (n + 2 * width)),
        name="species_compute",
    )(*operands)


def operator_rows(operators, count, row, columns):
    width = operators.shape[1] // count
    rows = lax.dynamic_slice_in_dim(operators, row * width, width, axis=1)
    parts = [lax.dynamic_slice_in_dim(rows, c * width, width, axis=2) for c in columns]
    return jnp.concatenate(parts, axis=2).reshape(2 * width, count * width)


MESH = pl.DeviceIdType.MESH
ROWS = 4
WINDOW = 4
TURNED = 4
SERVED = 3
SENT = 3


def local(src, dst, sem):
    return pltpu.make_async_copy(src, dst, sem)


def remote(src, dst, sent, got, **to):
    return pltpu.make_async_remote_copy(src, dst, sent, got, device_id=to, device_id_type=MESH)


def exchange_kernel(
    rows_n, cols_n, x_ops, y_ops, species, flow, sp_out, fl_out, gathered,
    weights, lines, own_v, own_o, served_o, t_in, t_scratch, t_out, g_v, sp_scratch, sp_o,
    lines_sem, sent_sem, own_sem, own_o_sem, served_sem, flow_sem,
    t_in_sem, t_out_sem, g_sem, copy_sem, sp_o_sem, sp_sem,
):
    me, col = lax.axis_index("row"), lax.axis_index("col")
    kinds, width_x, width_y, depth = flow.shape
    partner, far, mirror = col + 1 - 2 * (col % 2), (col + 2) % 4, 3 - col
    inner = jnp.logical_and(col >= 1, col <= 2)
    outer = jnp.logical_not(inner)
    per = width_x // ROWS
    steps = kinds * per
    tile = width_y // rows_n
    units = kinds * rows_n
    turns = -(-4 * units // steps)
    first = steps // 6
    spread = steps - first - steps // 12

    barrier = pltpu.get_barrier_semaphore()
    for i in range(1, rows_n):
        pl.semaphore_signal(
            barrier, inc=1, device_id={"row": (me + i) % rows_n}, device_id_type=MESH
        )
    for i in range(1, cols_n):
        pl.semaphore_signal(
            barrier, inc=1, device_id={"col": (col + i) % cols_n}, device_id_type=MESH
        )
    pl.semaphore_wait(barrier, rows_n + cols_n - 2)

    def rows_of(ref, k):
        return ref.at[k // per, pl.ds((k % per) * ROWS, ROWS)]

    def pairs_of(ref, k):
        return ref.at[k // per, :, pl.ds((k % per) * ROWS, ROWS)]

    def piece(role, k, slot, to):
        at = lines.at[role, pl.ds(k * ROWS, ROWS)]
        return remote(
            rows_of(flow, k), at, sent_sem.at[min(role, 1), slot], lines_sem.at[role, k], col=to
        )

    def send(k):
        @pl.when(outer)
        def _():
            piece(0, k, k % WINDOW, partner).start()
            piece(1, k, k % WINDOW, far).start()

        @pl.when(inner)
        def _():
            piece(2, k, k % WINDOW, mirror).start()

    def sent(k):
        piece(1, k, k % WINDOW, far).wait_send()

        @pl.when(outer)
        def _():
            piece(0, k, k % WINDOW, partner).wait_send()

    def load_own(k):
        return local(rows_of(flow, k), own_v.at[k % 2], own_sem.at[k % 2])

    def store_own(k):
        return local(own_o.at[k % 2], pairs_of(fl_out, k), own_o_sem.at[k % 2])

    def serve(k):
        return remote(
            served_o.at[k % SERVED], pairs_of(fl_out, k), served_sem.at[k % SERVED],
            flow_sem.at[k // per], col=partner,
        )

    def load_turn(m):
        s, r = m // rows_n, (me + 1 + m % rows_n) % rows_n
        return local(species.at[s, :, pl.ds(r * tile, tile)], t_in.at[m % 2], t_in_sem.at[m % 2])

    def send_turn(m):
        s, r = m // rows_n, (me + 1 + m % rows_n) % rows_n
        return remote(
            t_out.at[m % TURNED], gathered.at[s, me], t_out_sem.at[m % TURNED], g_sem.at[s], row=r
        )

    def send_species(u):
        s, r = u // rows_n, (me + 1 + u % rows_n) % rows_n
        return remote(
            sp_o.at[u % SENT], sp_out.at[s, :, :, pl.ds(me * tile, tile)],
            sp_o_sem.at[u % SENT], sp_sem.at[s], row=r,
        )

    def away(m):
        return m % rows_n != rows_n - 1

    for k in range(WINDOW):
        send(k)
    load_turn(0).start()

    @pl.when(inner)
    def _():
        load_own(0).start()
        for c, g in enumerate((col, partner, far, mirror)):
            for o, home in enumerate((col, partner)):
                for d in range(2):
                    weights[pl.ds((2 * o + d) * width_y, width_y), pl.ds(c * width_y, width_y)] = (
                        y_ops[
                            d,
                            pl.ds(pl.multiple_of(home * width_y, width_y), width_y),
                            pl.ds(pl.multiple_of(g * width_y, width_y), width_y),
                        ]
                    )

    def turn_step(m):
        load_turn(m).wait()

        @pl.when(m + 1 < units)
        def _():
            load_turn(m + 1).start()

        @pl.when(jnp.logical_and(m >= TURNED, away(m - TURNED)))
        def _():
            send_turn(m - TURNED).wait_send()

        for h in range(depth // 128):
            part = t_in[m % 2, :, :, h * 128 : (h + 1) * 128].astype(jnp.float32)
            t_scratch[h] = part.reshape(width_x * tile, 128)
        for y in range(tile):
            for h in range(depth // 128):
                t_out[m % TURNED, y, :, h * 128 : (h + 1) * 128] = t_scratch[
                    h, pl.ds(y, width_x, stride=tile), :
                ].astype(jnp.bfloat16)

        @pl.when(away(m))
        def _():
            send_turn(m).start()

        @pl.when(jnp.logical_not(away(m)))
        def _():
            copy = local(t_out.at[m % TURNED], gathered.at[m // rows_n, me], copy_sem)
            copy.start()
            copy.wait()

    def species_step(u):
        s, r = u // rows_n, (me + 1 + u % rows_n) % rows_n

        @pl.when(u % rows_n == 0)
        def _():
            got = gathered.at[s, pl.ds(0, rows_n - 1)]
            remote(got, got, copy_sem, g_sem.at[s], row=r).wait_recv()
            copy = local(gathered.at[s], g_v, copy_sem)
            copy.start()
            copy.wait()

        @pl.when(jnp.logical_and(u >= SENT, away(u - SENT)))
        def _():
            send_species(u - SENT).wait_send()

        at = pl.ds(pl.multiple_of(r * width_x, width_x), width_x)
        for y in range(tile):
            block = jnp.concatenate([g_v[g, y] for g in range(rows_n)], axis=0)
            w = jnp.concatenate([x_ops[0, at], x_ops[1, at]], axis=0)
            out = jnp.dot(w, block, preferred_element_type=jnp.float32)
            for h in range(depth // 128):
                sp_scratch[h, pl.ds(y, 2 * width_x, stride=tile), :] = out[
                    :, h * 128 : (h + 1) * 128
                ]
        for h in range(depth // 128):
            for d in range(2):
                part = sp_scratch[h, d * width_x * tile : (d + 1) * width_x * tile, :]
                sp_o[u % SENT, d, :, :, h * 128 : (h + 1) * 128] = part.reshape(
                    width_x, tile, 128
                ).astype(jnp.bfloat16)

        @pl.when(away(u))
        def _():
            send_species(u).start()

        @pl.when(jnp.logical_not(away(u)))
        def _():
            copy = local(
                sp_o.at[u % SENT], sp_out.at[s, :, :, pl.ds(me * tile, tile)], copy_sem
            )
            copy.start()
            copy.wait()

    def flow_step(k):
        for role, source in enumerate((partner, far, mirror)):
            piece(role, k, k % WINDOW, source).wait_recv()
        load_own(k).wait()

        @pl.when(k + 1 < steps)
        def _():
            load_own(k + 1).start()

        @pl.when(k >= 2)
        def _():
            store_own(k - 2).wait()

        @pl.when(k >= SERVED)
        def _():
            serve(k - SERVED).wait_send()

        for x in range(ROWS):
            block = jnp.concatenate(
                [own_v[k % 2, x]] + [lines[j, k * ROWS + x] for j in range(3)], axis=0
            )
            out = jnp.dot(weights[...], block, preferred_element_type=jnp.float32)
            out = out.astype(jnp.bfloat16)
            for d in range(2):
                served_o[k % SERVED, d, x] = out[(2 + d) * width_y : (3 + d) * width_y]
                own_o[k % 2, d, x] = out[d * width_y : (d + 1) * width_y]
        serve(k).start()
        store_own(k).start()

    @pl.loop(0, steps)
    def _(k):
        for i in range(turns):

            @pl.when(k * turns + i < units)
            def _():
                turn_step(k * turns + i)

        past = (k - first) * units
        u = past // spread

        @pl.when(
            jnp.logical_and(
                jnp.logical_and(k >= first, u < units), u != (past + units) // spread
            )
        )
        def _():
            species_step(u)

        @pl.when(inner)
        def _():
            flow_step(k)

        sent(k)

        @pl.when(k + WINDOW < steps)
        def _():
            send(k + WINDOW)

    for m in range(units - TURNED, units):
        if m % rows_n != rows_n - 1:
            send_turn(m).wait_send()
    for u in range(units - SENT, units):
        if u % rows_n != rows_n - 1:
            send_species(u).wait_send()
    for s in range(kinds):
        got = sp_out.at[s, :, :, pl.ds(0, width_y - tile)]
        remote(got, got, copy_sem, sp_sem.at[s], row=me).wait_recv()

    @pl.when(inner)
    def _():
        for k in range(steps - 2, steps):
            store_own(k).wait()
        for k in range(steps - SERVED, steps):
            serve(k).wait_send()

    @pl.when(outer)
    def _():
        for s in range(kinds):
            got = fl_out.at[s]
            remote(got, got, copy_sem, flow_sem.at[s], col=partner).wait_recv()


def exchange(rows_n, cols_n, species, flow, x_operators, y_operators):
    kinds, width_x, width_y, depth = flow.shape
    tile = width_y // rows_n
    steps = kinds * width_x // ROWS
    whole = jax.ShapeDtypeStruct((kinds, 2, width_x, width_y, depth), jnp.bfloat16)
    kept = jax.ShapeDtypeStruct((kinds, rows_n, tile, width_x, depth), jnp.bfloat16)
    any_space = pl.BlockSpec(memory_space=pl.ANY)
    in_vmem = pl.BlockSpec(memory_space=pltpu.VMEM)
    dma = pltpu.SemaphoreType.DMA

    def vmem(*shape, dtype=jnp.bfloat16):
        return pltpu.VMEM(shape, dtype)

    halves = depth // 128
    species_out, flow_out, _ = pl.pallas_call(
        functools.partial(exchange_kernel, rows_n, cols_n),
        in_specs=[in_vmem, in_vmem, any_space, any_space],
        out_specs=[any_space] * 3,
        out_shape=[whole, whole, kept],
        scratch_shapes=[
            vmem(4 * width_y, cols_n * width_y),
            vmem(3, kinds * width_x, width_y, depth),
            vmem(2, ROWS, width_y, depth),
            vmem(2, 2, ROWS, width_y, depth),
            vmem(SERVED, 2, ROWS, width_y, depth),
            vmem(2, width_x, tile, depth),
            vmem(halves, width_x * tile, 128, dtype=jnp.float32),
            vmem(TURNED, tile, width_x, depth),
            vmem(rows_n, tile, width_x, depth),
            vmem(halves, 2 * width_x * tile, 128, dtype=jnp.float32),
            vmem(SENT, 2, width_x, tile, depth),
            dma((3, steps)),
            dma((2, WINDOW)),
            dma((2,)),
            dma((2,)),
            dma((SERVED,)),
            dma((kinds,)),
            dma((2,)),
            dma((TURNED,)),
            dma((kinds,)),
            dma,
            dma((SENT,)),
            dma((kinds,)),
        ],
        compiler_params=pltpu.CompilerParams(
            collective_id=0, has_side_effects=True, vmem_limit_bytes=63 * 1024 * 1024
        ),
        cost_estimate=cost(
            16 * kinds * width_x * width_y * cols_n * width_y * depth,
            12 * kinds * width_x * width_y * depth,
        ),
        name="exchange",
    )(x_operators, y_operators, species, flow)
    return species_out, flow_out


def body(rows_n, cols_n, species, flow, x_operators, y_operators):
    kinds, width_x, width_y, depth = species.shape
    out_shape = (kinds, 2, width_x, width_y, depth)
    if cols_n == 4 and width_y == 16 * rows_n and width_x % 16 == 0:
        return exchange(rows_n, cols_n, species, flow, x_operators, y_operators)

    quarter, half = cols_n // 4, cols_n // 2
    inner = [quarter + i for i in range(half)]
    outer = [i if i < quarter else i + half for i in range(half)]
    at = jnp.clip(lax.axis_index("col") - quarter, 0, half - 1)

    def inner_of(i):
        return quarter + i

    def outer_of(i):
        return jnp.where(i < quarter, i, i + half)

    plans, columns = [], [inner_of(at)]
    for k in range(half):
        plans.append([(outer[i], inner[(i + k) % half]) for i in range(half)])
        columns.append(outer_of((at - k) % half))
    for k in range(1, half):
        plans.append([(inner[i], inner[(i + k) % half]) for i in range(half)])
        columns.append(inner_of((at - k) % half))
    back = [(inner[i], outer[i]) for i in range(half)]
    y_weights = jnp.concatenate(
        [operator_rows(y_operators, cols_n, o, columns) for o in (inner_of(at), outer_of(at))]
    )

    row = lax.axis_index("row")
    x_weights = lax.dynamic_slice_in_dim(x_operators, row * width_x, width_x, axis=1)
    x_weights = x_weights.reshape(2 * width_x, rows_n * width_x)
    lines = [lax.all_gather(turn(species, s), "row") for s in range(kinds)]

    flow_rows = width_x // FLOW_SPLITS
    chunks = [(s, c * flow_rows) for s in range(kinds) for c in range(FLOW_SPLITS)]
    pieces = [flow[s, start : start + flow_rows] for s, start in chunks[:AHEAD]]
    received = [[lax.ppermute(piece, "col", plan) for plan in plans] for piece in pieces]

    when = {((s + 1) * len(chunks)) // kinds + LAG: s for s in range(kinds)}
    species_out, flow_out, results, order = None, None, [], []

    def multiply(s, after):
        return species_compute(out_shape, x_weights, lines[s], species_out, s, 0, after)

    def pick(k):
        s, start = chunks[k]
        return flow_pick(out_shape, *results[k], flow_out, s, start, flow_rows, cols_n)

    for k, (s, start) in enumerate(chunks):
        tokens = order
        if k in when:
            species_out, token = multiply(when[k], tokens)
            tokens = [token]
        ahead = chunks[k + AHEAD] if k + AHEAD < len(chunks) else None
        own, served, *piece = flow_compute(
            y_weights, flow, received[k], s, start, flow_rows, ahead, tokens
        )
        received.extend([lax.ppermute(p, "col", plan) for plan in plans] for p in piece)
        results.append((own, lax.ppermute(served, "col", back)))
        order = []
        if k >= BEHIND:
            flow_out, token = pick(k - BEHIND)
            order = [token]
    for k, s in when.items():
        if k >= len(chunks):
            species_out, token = multiply(s, order)
            order = [token]
    for k in range(len(chunks) - BEHIND, len(chunks)):
        flow_out, _ = pick(k)
    return (species_out, flow_out)


def solution(mesh):
    placed = (P(None, "row", "col", None), P(None, "row", "col", None), P(), P())
    return jax.shard_map(
        functools.partial(body, mesh.shape["row"], mesh.shape["col"]),
        mesh=mesh,
        in_specs=placed,
        out_specs=(P(None, None, "row", "col", None), P(None, None, "row", "col", None)),
        check_vma=False,
    )
```

```python
import functools

import jax
import jax.numpy as jnp
from jax import lax
from jax.experimental import pallas as pl
from jax.experimental.pallas import tpu as pltpu
from jax.sharding import PartitionSpec as P


FLOW_SPLITS = 4
AHEAD = 3
BEHIND = 3
LAG = 1
VMEM = 56 * 1024 * 1024


def params():
    return pltpu.CompilerParams(vmem_limit_bytes=VMEM)


def cost(flops, moved):
    return pl.CostEstimate(flops=flops, bytes_accessed=moved, transcendentals=0)


TOKEN = jax.ShapeDtypeStruct((8, 128), jnp.float32)
TOKEN_SPEC = pl.BlockSpec((8, 128), lambda g: (0, 0))
ANY_SPEC = pl.BlockSpec(memory_space=pl.ANY)


def flow_kernel(count, ahead, w_ref, *refs):
    sources, (own_ref, served_ref) = refs[:count], refs[-2 - ahead :][:2]
    width = own_ref.shape[3]
    if ahead:
        refs[-1][...] = refs[count][0]

    @pl.loop(0, own_ref.shape[2])
    def _(x):
        lines = jnp.concatenate(
            [s[0, x] if len(s.shape) == 4 else s[x] for s in sources], axis=0
        )
        out = jnp.dot(w_ref[...], lines, preferred_element_type=jnp.float32)
        out = out.astype(jnp.bfloat16)
        for d in range(2):
            own_ref[0, d, x] = out[d * width : (d + 1) * width]
            served_ref[d, x] = out[(2 + d) * width : (3 + d) * width]


def flow_compute(weights, flow, received, s, start, rows, ahead, tokens):
    _, _, width, depth = flow.shape
    tile = min(rows, 4)
    block = pl.BlockSpec((tile, width, depth), lambda g: (g, 0, 0))

    def piece_of(s, start):
        return pl.BlockSpec((1, tile, width, depth), lambda g: (s, start // tile + g, 0, 0))

    n = weights.shape[1]
    later = [] if ahead is None else [ahead]
    return pl.pallas_call(
        functools.partial(flow_kernel, 1 + len(received), len(later)),
        grid=(rows // tile,),
        in_specs=[pl.BlockSpec(weights.shape, lambda g: (0, 0)), piece_of(s, start)]
        + [block] * len(received)
        + [piece_of(*at) for at in later]
        + [ANY_SPEC] * len(tokens),
        out_specs=[
            pl.BlockSpec((1, 2, tile, width, depth), lambda g: (0, 0, g, 0, 0)),
            pl.BlockSpec((2, tile, width, depth), lambda g: (0, g, 0, 0)),
        ]
        + [block] * len(later),
        out_shape=[
            jax.ShapeDtypeStruct((1, 2, rows, width, depth), jnp.bfloat16),
            jax.ShapeDtypeStruct((2, rows, width, depth), jnp.bfloat16),
        ]
        + [jax.ShapeDtypeStruct((rows, width, depth), jnp.bfloat16)] * len(later),
        compiler_params=params(),
        cost_estimate=cost(8 * rows * width * n * depth, 2 * rows * depth * (n + 4 * width)),
        name="flow_compute",
    )(weights, flow, *received, *[flow for _ in later], *tokens)


def pick_kernel(count, quarter, own_ref, got_ref, *refs):
    out_ref, token_ref = refs[-2:]
    me = lax.axis_index("col")
    inner = jnp.logical_and(me >= quarter, me < count - quarter)
    token_ref[...] = jnp.zeros_like(token_ref)

    @pl.when(inner)
    def _():
        out_ref[...] = own_ref[...]

    @pl.when(jnp.logical_not(inner))
    def _():
        out_ref[0] = got_ref[...]


def flow_pick(shape, own, got, whole, s, start, rows, count):
    tile = min(rows, 4)
    width, depth = shape[3:]
    operands = (own, got) + (() if whole is None else (whole,))
    return pl.pallas_call(
        functools.partial(pick_kernel, count, count // 4),
        grid=(rows // tile,),
        in_specs=[
            pl.BlockSpec((1, 2, tile, width, depth), lambda g: (0, 0, g, 0, 0)),
            pl.BlockSpec((2, tile, width, depth), lambda g: (0, g, 0, 0)),
        ]
        + [ANY_SPEC] * (len(operands) - 2),
        out_specs=[
            pl.BlockSpec(
                (1, 2, tile, width, depth), lambda g: (s, 0, start // tile + g, 0, 0)
            ),
            TOKEN_SPEC,
        ],
        out_shape=[jax.ShapeDtypeStruct(shape, jnp.bfloat16), TOKEN],
        input_output_aliases={2: 0} if whole is not None else {},
        compiler_params=params(),
        cost_estimate=cost(0, 12 * rows * width * depth),
        name="flow_pick",
    )(*operands)


def turn_kernel(in_ref, out_ref, scratch):
    _, width, tile, depth = in_ref.shape
    for h in range(depth // 128):
        part = in_ref[0, :, :, h * 128 : (h + 1) * 128].astype(jnp.float32)
        scratch[h] = part.reshape(width * tile, 128)
    for y in range(tile):
        for h in range(depth // 128):
            out_ref[y, :, h * 128 : (h + 1) * 128] = scratch[
                h, pl.ds(y, width, stride=tile), :
            ].astype(jnp.bfloat16)


def turn(species, s):
    _, width, rows, depth = species.shape
    tile = 16
    return pl.pallas_call(
        turn_kernel,
        grid=(rows // tile,),
        in_specs=[pl.BlockSpec((1, width, tile, depth), lambda g: (s, 0, g, 0))],
        out_specs=pl.BlockSpec((tile, width, depth), lambda g: (g, 0, 0)),
        out_shape=jax.ShapeDtypeStruct((rows, width, depth), jnp.bfloat16),
        scratch_shapes=[pltpu.VMEM((depth // 128, width * tile, 128), jnp.float32)],
        compiler_params=params(),
        cost_estimate=cost(0, 4 * rows * width * depth),
        name="turn",
    )(species)


def species_kernel(w_ref, lines_ref, *refs):
    out_ref, token_ref, scratch = refs[-3:]
    _, _, width, tile, depth = out_ref.shape
    token_ref[...] = jnp.zeros_like(token_ref)

    for y in range(tile):
        lines = jnp.concatenate([lines_ref[k, y] for k in range(lines_ref.shape[0])], axis=0)
        out = jnp.dot(w_ref[...], lines, preferred_element_type=jnp.float32)
        for h in range(depth // 128):
            scratch[h, pl.ds(y, 2 * width, stride=tile), :] = out[:, h * 128 : (h + 1) * 128]
    for h in range(depth // 128):
        for d in range(2):
            part = scratch[h, d * width * tile : (d + 1) * width * tile, :]
            out_ref[0, d, :, :, h * 128 : (h + 1) * 128] = part.reshape(
                width, tile, 128
            ).astype(jnp.bfloat16)


def species_compute(shape, weights, lines, whole, s, start, tokens):
    _, _, width, _, depth = shape
    count, rows = lines.shape[:2]
    tile = 16
    operands = (weights, lines) + (() if whole is None else (whole,)) + tuple(tokens)
    n = weights.shape[1]
    return pl.pallas_call(
        species_kernel,
        grid=(rows // tile,),
        in_specs=[
            pl.BlockSpec(weights.shape, lambda g: (0, 0)),
            pl.BlockSpec((count, tile, width, depth), lambda g: (0, g, 0, 0)),
        ]
        + [ANY_SPEC] * (len(operands) - 2),
        out_specs=[
            pl.BlockSpec(
                (1, 2, width, tile, depth), lambda g: (s, 0, 0, start // tile + g, 0)
            ),
            TOKEN_SPEC,
        ],
        out_shape=[jax.ShapeDtypeStruct(shape, jnp.bfloat16), TOKEN],
        scratch_shapes=[pltpu.VMEM((depth // 128, 2 * width * tile, 128), jnp.float32)],
        input_output_aliases={2: 0} if whole is not None else {},
        compiler_params=params(),
        cost_estimate=cost(4 * rows * width * n * depth, 2 * rows * depth * (n + 2 * width)),
        name="species_compute",
    )(*operands)


def operator_rows(operators, count, row, columns):
    width = operators.shape[1] // count
    rows = lax.dynamic_slice_in_dim(operators, row * width, width, axis=1)
    parts = [lax.dynamic_slice_in_dim(rows, c * width, width, axis=2) for c in columns]
    return jnp.concatenate(parts, axis=2).reshape(2 * width, count * width)


MESH = pl.DeviceIdType.MESH
ROWS = 1
WINDOW = 8
RING = 20
TURNED = 8
SERVED = 6
SENT = 8
BLOCK = 32
SLOTS = 8
NEAR = 1


def local(src, dst, sem):
    return pltpu.make_async_copy(src, dst, sem)


def remote(src, dst, sent, got, **to):
    return pltpu.make_async_remote_copy(src, dst, sent, got, device_id=to, device_id_type=MESH)


def exchange_kernel(
    rows_n, cols_n, x_ops, y_ops, species, flow, sp_far, sp_near, fl_out, gathered,
    weights, lines, own_v, served_o, t_in, t_scratch, t_out, g_v, sp_scratch, sp_o,
    lines_sem, sent_sem, credit, own_sem, served_sem, flow_sem,
    t_in_sem, t_out_sem, g_sem, copy_sem, sp_o_sem, sp_sem,
):
    me, col = lax.axis_index("row"), lax.axis_index("col")
    kinds, width_x, width_y, depth = flow.shape
    partner, far, mirror = col + 1 - 2 * (col % 2), (col + 2) % 4, 3 - col
    inner = jnp.logical_and(col >= 1, col <= 2)
    outer = jnp.logical_not(inner)
    per = width_x // ROWS
    steps = kinds * per
    tile = width_y // rows_n
    units = kinds * rows_n
    first = 5 * steps // 16
    spread = steps - first - steps // 16

    barrier = pltpu.get_barrier_semaphore()
    for i in range(1, rows_n):
        pl.semaphore_signal(
            barrier, inc=1, device_id={"row": (me + i) % rows_n}, device_id_type=MESH
        )
    for i in range(1, cols_n):
        pl.semaphore_signal(
            barrier, inc=1, device_id={"col": (col + i) % cols_n}, device_id_type=MESH
        )
    pl.semaphore_wait(barrier, rows_n + cols_n - 2)

    def rows_of(ref, k):
        return ref.at[k // per, pl.ds((k % per) * ROWS, ROWS)]

    def pairs_of(ref, k):
        return ref.at[k // per, :, pl.ds((k % per) * ROWS, ROWS)]

    def piece(role, k, slot, to):
        at = lines.at[role, k % RING]
        return remote(
            rows_of(flow, k), at, sent_sem.at[min(role, 1), slot], lines_sem.at[role, k % RING],
            col=to,
        )

    def send(k):
        @pl.when(jnp.logical_and(outer, k >= RING))
        def _():
            pl.semaphore_wait(credit.at[0], 1)

        @pl.when(k >= RING)
        def _():
            pl.semaphore_wait(credit.at[1], 1)

        @pl.when(outer)
        def _():
            piece(0, k, k % WINDOW, partner).start()
            piece(1, k, k % WINDOW, far).start()

        @pl.when(inner)
        def _():
            piece(2, k, k % WINDOW, mirror).start()

    def sent(k):
        piece(1, k, k % WINDOW, far).wait_send()

        @pl.when(outer)
        def _():
            piece(0, k, k % WINDOW, partner).wait_send()

    def load_own(k):
        return local(rows_of(flow, k), own_v.at[k % 2], own_sem.at[k % 2])

    def serve(k):
        return remote(
            served_o.at[k % SERVED], pairs_of(fl_out, k), served_sem.at[k % SERVED],
            flow_sem.at[k // per], col=partner,
        )

    def load_turn(m):
        s, r = m // rows_n, (me + 1 + m % rows_n) % rows_n
        return local(species.at[s, :, pl.ds(r * tile, tile)], t_in.at[m % 2], t_in_sem.at[m % 2])

    def send_turn(m):
        s, r = m // rows_n, (me + 1 + m % rows_n) % rows_n
        return remote(
            t_out.at[m % TURNED], gathered.at[s, me], t_out_sem.at[m % TURNED], g_sem.at[s], row=r
        )

    def send_species(u, part=sp_far, s=0):
        r = (me + 1 + u % rows_n) % rows_n
        return remote(
            sp_o.at[u % SENT], part.at[s, :, :, pl.ds(me * tile, tile)],
            sp_o_sem.at[u % SENT], sp_sem.at[u // rows_n], row=r,
        )

    def away(m):
        return m % rows_n != rows_n - 1

    @pl.loop(0, WINDOW)
    def _(k):
        send(k)

    load_turn(0).start()

    @pl.when(inner)
    def _():
        load_own(0).start()
        for c, g in enumerate((col, partner, far, mirror)):
            for o, home in enumerate((col, partner)):
                for d in range(2):
                    weights[pl.ds((2 * o + d) * width_y, width_y), pl.ds(c * width_y, width_y)] = (
                        y_ops[
                            d,
                            pl.ds(pl.multiple_of(home * width_y, width_y), width_y),
                            pl.ds(pl.multiple_of(g * width_y, width_y), width_y),
                        ]
                    )

    def turn_step(m):
        load_turn(m).wait()

        @pl.when(m + 1 < units)
        def _():
            load_turn(m + 1).start()

        @pl.when(jnp.logical_and(m >= TURNED, away(m - TURNED)))
        def _():
            send_turn(m - TURNED).wait_send()

        for h in range(depth // 128):
            part = t_in[m % 2, :, :, h * 128 : (h + 1) * 128].astype(jnp.float32)
            t_scratch[h] = part.reshape(width_x * tile, 128)
        for y in range(tile):
            for h in range(depth // 128):
                t_out[m % TURNED, y, :, h * 128 : (h + 1) * 128] = t_scratch[
                    h, pl.ds(y, width_x, stride=tile), :
                ].astype(jnp.bfloat16)

        @pl.when(away(m))
        def _():
            send_turn(m).start()

        @pl.when(jnp.logical_not(away(m)))
        def _():
            copy = local(t_out.at[m % TURNED], gathered.at[m // rows_n, me], copy_sem)
            copy.start()
            copy.wait()

    def species_step(u):
        s, r = u // rows_n, (me + 1 + u % rows_n) % rows_n

        @pl.when(u % rows_n == 0)
        def _():
            got = gathered.at[s, pl.ds(0, rows_n - 1)]
            remote(got, got, copy_sem, g_sem.at[s], row=r).wait_recv()
            copy = local(gathered.at[s], g_v, copy_sem)
            copy.start()
            copy.wait()

        @pl.when(jnp.logical_and(u >= SENT, away(u - SENT)))
        def _():
            send_species(u - SENT).wait_send()

        at = pl.ds(pl.multiple_of(r * width_x, width_x), width_x)
        for y in range(tile):
            block = jnp.concatenate([g_v[g, y] for g in range(rows_n)], axis=0)
            w = jnp.concatenate([x_ops[0, at], x_ops[1, at]], axis=0)
            out = jnp.dot(w, block, preferred_element_type=jnp.float32)
            for h in range(depth // 128):
                sp_scratch[h, pl.ds(y, 2 * width_x, stride=tile), :] = out[
                    :, h * 128 : (h + 1) * 128
                ]
        for h in range(depth // 128):
            for d in range(2):
                part = sp_scratch[h, d * width_x * tile : (d + 1) * width_x * tile, :]
                sp_o[u % SENT, d, :, :, h * 128 : (h + 1) * 128] = part.reshape(
                    width_x, tile, 128
                ).astype(jnp.bfloat16)

        for part, at, here in ((sp_near, s, s < NEAR), (sp_far, s - NEAR, s >= NEAR)):

            @pl.when(jnp.logical_and(away(u), here))
            def _():
                send_species(u, part, at).start()

            @pl.when(jnp.logical_and(jnp.logical_not(away(u)), here))
            def _():
                copy = local(
                    sp_o.at[u % SENT], part.at[at, :, :, pl.ds(me * tile, tile)], copy_sem
                )
                copy.start()
                copy.wait()

    def flow_step(k):
        for role, source in enumerate((partner, far, mirror)):
            piece(role, k, k % WINDOW, source).wait_recv()
        load_own(k).wait()

        @pl.when(k + 1 < steps)
        def _():
            load_own(k + 1).start()

        @pl.when(k >= SERVED)
        def _():
            serve(k - SERVED).wait_send()

        for x in range(ROWS):
            block = jnp.concatenate(
                [own_v[k % 2, x]] + [lines[j, k % RING, x] for j in range(3)], axis=0
            )
            out = jnp.dot(weights[...], block, preferred_element_type=jnp.float32)
            out = out.astype(jnp.bfloat16)
            for d in range(2):
                served_o[k % SERVED, d, x] = out[(2 + d) * width_y : (3 + d) * width_y]
                fl_out[k // per, d, k % per * ROWS + x] = out[d * width_y : (d + 1) * width_y]
        serve(k).start()

        @pl.when(k + RING < steps)
        def _():
            for i, source in enumerate((partner, far, mirror)):
                pl.semaphore_signal(
                    credit.at[min(i, 1)], inc=1, device_id={"col": source}, device_id_type=MESH
                )

    @pl.loop(0, steps)
    def _(k):
        m = k * units // first

        @pl.when(jnp.logical_and(m < units, m != (k + 1) * units // first))
        def _():
            turn_step(m)

        past = (k - first) * units
        u = past // spread

        @pl.when(
            jnp.logical_and(
                jnp.logical_and(k >= first, u < units), u != (past + units) // spread
            )
        )
        def _():
            species_step(u)

        @pl.when(inner)
        def _():
            flow_step(k)

        sent(k)

        @pl.when(k + WINDOW < steps)
        def _():
            send(k + WINDOW)

    for m in range(units - TURNED, units):
        if m % rows_n != rows_n - 1:
            send_turn(m).wait_send()
    for u in range(units - SENT, units):
        if u % rows_n != rows_n - 1:
            send_species(u).wait_send()
    for s in range(kinds):
        part = sp_near.at[s] if s < NEAR else sp_far.at[s - NEAR]
        got = part.at[:, :, pl.ds(0, width_y - tile)]
        remote(got, got, copy_sem, sp_sem.at[s], row=me).wait_recv()

    @pl.when(inner)
    def _():
        for k in range(steps - SERVED, steps):
            serve(k).wait_send()

    @pl.when(outer)
    def _():
        for s in range(kinds):
            got = fl_out.at[s]
            remote(got, got, copy_sem, flow_sem.at[s], col=partner).wait_recv()


def settle_kernel(far, near, flow, sp_out, fl_out, held, in_sem, out_sem, near_sem):
    slots, rows = held.shape[:2]
    blocks, skip = far.shape[0] // rows, near.shape[0]

    def load(j):
        return local(far.at[pl.ds(j * rows, rows)], held.at[j % slots], in_sem.at[j % slots])

    def store(j):
        result = sp_out.at[pl.ds(skip + j * rows, rows)]
        return local(held.at[j % slots], result, out_sem.at[j % slots])

    ahead = slots // 2
    for j in range(min(ahead, blocks)):
        load(j).start()
    whole = [
        local(near, sp_out.at[pl.ds(0, skip)], near_sem.at[0]),
        local(flow, fl_out, near_sem.at[1]),
    ]
    for copy in whole:
        copy.start()
    for j in range(blocks):
        load(j).wait()
        store(j).start()
        if j + ahead < blocks:
            if j + ahead >= slots:
                store(j + ahead - slots).wait()
            load(j + ahead).start()
    for j in range(max(0, blocks - slots), blocks):
        store(j).wait()
    for copy in whole:
        copy.wait()


def settle(far, near, flow):
    shape = flow.shape
    far, near, flow = (a.reshape((-1,) + shape[3:]) for a in (far, near, flow))
    rows = min(far.shape[0], BLOCK)
    in_vmem = pl.BlockSpec(memory_space=pltpu.VMEM)
    results = pl.pallas_call(
        settle_kernel,
        in_specs=[ANY_SPEC, in_vmem, in_vmem],
        out_specs=[ANY_SPEC] * 2,
        out_shape=[jax.ShapeDtypeStruct(flow.shape, flow.dtype)] * 2,
        scratch_shapes=[
            pltpu.VMEM((SLOTS, rows) + shape[3:], jnp.bfloat16),
            pltpu.SemaphoreType.DMA((SLOTS,)),
            pltpu.SemaphoreType.DMA((SLOTS,)),
            pltpu.SemaphoreType.DMA((2,)),
        ],
        compiler_params=pltpu.CompilerParams(vmem_limit_bytes=20 * 1024 * 1024),
        cost_estimate=cost(0, 4 * far.size + 2 * near.size + 2 * flow.size),
        name="settle",
    )(far, *[pltpu.with_memory_space_constraint(a, pltpu.VMEM) for a in (near, flow)])
    return tuple(r.reshape(shape) for r in results)


def exchange(rows_n, cols_n, species, flow, x_operators, y_operators):
    kinds, width_x, width_y, depth = flow.shape
    tile = width_y // rows_n
    shape = (2, width_x, width_y, depth)
    kept = jax.ShapeDtypeStruct((kinds, rows_n, tile, width_x, depth), jnp.bfloat16)
    any_space = pl.BlockSpec(memory_space=pl.ANY)
    in_vmem = pl.BlockSpec(memory_space=pltpu.VMEM)
    dma = pltpu.SemaphoreType.DMA

    def vmem(*shape, dtype=jnp.bfloat16):
        return pltpu.VMEM(shape, dtype)

    halves = depth // 128
    far, near, flow_out, _ = pl.pallas_call(
        functools.partial(exchange_kernel, rows_n, cols_n),
        in_specs=[in_vmem, in_vmem, any_space, any_space],
        out_specs=[any_space, in_vmem, in_vmem, any_space],
        out_shape=[
            jax.ShapeDtypeStruct((kinds - NEAR,) + shape, jnp.bfloat16),
            pltpu.VMEM((NEAR,) + shape, jnp.bfloat16),
            pltpu.VMEM((kinds,) + shape, jnp.bfloat16),
            kept,
        ],
        scratch_shapes=[
            vmem(4 * width_y, cols_n * width_y),
            vmem(3, RING, ROWS, width_y, depth),
            vmem(2, ROWS, width_y, depth),
            vmem(SERVED, 2, ROWS, width_y, depth),
            vmem(2, width_x, tile, depth),
            vmem(halves, width_x * tile, 128, dtype=jnp.float32),
            vmem(TURNED, tile, width_x, depth),
            vmem(rows_n, tile, width_x, depth),
            vmem(halves, 2 * width_x * tile, 128, dtype=jnp.float32),
            vmem(SENT, 2, width_x, tile, depth),
            dma((3, RING)),
            dma((2, WINDOW)),
            pltpu.SemaphoreType.REGULAR((2,)),
            dma((2,)),
            dma((SERVED,)),
            dma((kinds,)),
            dma((2,)),
            dma((TURNED,)),
            dma((kinds,)),
            dma,
            dma((SENT,)),
            dma((kinds,)),
        ],
        compiler_params=pltpu.CompilerParams(
            collective_id=0, has_side_effects=True, vmem_limit_bytes=31 * 1024 * 1024
        ),
        cost_estimate=cost(
            16 * kinds * width_x * width_y * cols_n * width_y * depth,
            12 * kinds * width_x * width_y * depth,
        ),
        name="exchange",
    )(x_operators, y_operators, species, flow)
    return settle(far, near, flow_out)


def body(rows_n, cols_n, species, flow, x_operators, y_operators):
    kinds, width_x, width_y, depth = species.shape
    out_shape = (kinds, 2, width_x, width_y, depth)
    if cols_n == 4 and width_y == 16 * rows_n and width_x % 16 == 0:
        return exchange(rows_n, cols_n, species, flow, x_operators, y_operators)

    quarter, half = cols_n // 4, cols_n // 2
    inner = [quarter + i for i in range(half)]
    outer = [i if i < quarter else i + half for i in range(half)]
    at = jnp.clip(lax.axis_index("col") - quarter, 0, half - 1)

    def inner_of(i):
        return quarter + i

    def outer_of(i):
        return jnp.where(i < quarter, i, i + half)

    plans, columns = [], [inner_of(at)]
    for k in range(half):
        plans.append([(outer[i], inner[(i + k) % half]) for i in range(half)])
        columns.append(outer_of((at - k) % half))
    for k in range(1, half):
        plans.append([(inner[i], inner[(i + k) % half]) for i in range(half)])
        columns.append(inner_of((at - k) % half))
    back = [(inner[i], outer[i]) for i in range(half)]
    y_weights = jnp.concatenate(
        [operator_rows(y_operators, cols_n, o, columns) for o in (inner_of(at), outer_of(at))]
    )

    row = lax.axis_index("row")
    x_weights = lax.dynamic_slice_in_dim(x_operators, row * width_x, width_x, axis=1)
    x_weights = x_weights.reshape(2 * width_x, rows_n * width_x)
    lines = [lax.all_gather(turn(species, s), "row") for s in range(kinds)]

    flow_rows = width_x // FLOW_SPLITS
    chunks = [(s, c * flow_rows) for s in range(kinds) for c in range(FLOW_SPLITS)]
    pieces = [flow[s, start : start + flow_rows] for s, start in chunks[:AHEAD]]
    received = [[lax.ppermute(piece, "col", plan) for plan in plans] for piece in pieces]

    when = {((s + 1) * len(chunks)) // kinds + LAG: s for s in range(kinds)}
    species_out, flow_out, results, order = None, None, [], []

    def multiply(s, after):
        return species_compute(out_shape, x_weights, lines[s], species_out, s, 0, after)

    def pick(k):
        s, start = chunks[k]
        return flow_pick(out_shape, *results[k], flow_out, s, start, flow_rows, cols_n)

    for k, (s, start) in enumerate(chunks):
        tokens = order
        if k in when:
            species_out, token = multiply(when[k], tokens)
            tokens = [token]
        ahead = chunks[k + AHEAD] if k + AHEAD < len(chunks) else None
        own, served, *piece = flow_compute(
            y_weights, flow, received[k], s, start, flow_rows, ahead, tokens
        )
        received.extend([lax.ppermute(p, "col", plan) for plan in plans] for p in piece)
        results.append((own, lax.ppermute(served, "col", back)))
        order = []
        if k >= BEHIND:
            flow_out, token = pick(k - BEHIND)
            order = [token]
    for k, s in when.items():
        if k >= len(chunks):
            species_out, token = multiply(s, order)
            order = [token]
    for k in range(len(chunks) - BEHIND, len(chunks)):
        flow_out, _ = pick(k)
    return (species_out, flow_out)


def solution(mesh):
    placed = (P(None, "row", "col", None), P(None, "row", "col", None), P(), P())
    return jax.shard_map(
        functools.partial(body, mesh.shape["row"], mesh.shape["col"]),
        mesh=mesh,
        in_specs=placed,
        out_specs=(P(None, None, "row", "col", None), P(None, None, "row", "col", None)),
        check_vma=False,
    )
```

```python
import functools

import jax
import jax.numpy as jnp
from jax import lax
from jax.experimental import pallas as pl
from jax.experimental.pallas import tpu as pltpu
from jax.sharding import PartitionSpec as P


FLOW_SPLITS = 4
AHEAD = 3
BEHIND = 3
LAG = 1
VMEM = 56 * 1024 * 1024


def params():
    return pltpu.CompilerParams(vmem_limit_bytes=VMEM)


def cost(flops, moved):
    return pl.CostEstimate(flops=flops, bytes_accessed=moved, transcendentals=0)


TOKEN = jax.ShapeDtypeStruct((8, 128), jnp.float32)
TOKEN_SPEC = pl.BlockSpec((8, 128), lambda g: (0, 0))
ANY_SPEC = pl.BlockSpec(memory_space=pl.ANY)


def flow_kernel(count, ahead, w_ref, *refs):
    sources, (own_ref, served_ref) = refs[:count], refs[-2 - ahead :][:2]
    width = own_ref.shape[3]
    if ahead:
        refs[-1][...] = refs[count][0]

    @pl.loop(0, own_ref.shape[2])
    def _(x):
        lines = jnp.concatenate(
            [s[0, x] if len(s.shape) == 4 else s[x] for s in sources], axis=0
        )
        out = jnp.dot(w_ref[...], lines, preferred_element_type=jnp.float32)
        out = out.astype(jnp.bfloat16)
        for d in range(2):
            own_ref[0, d, x] = out[d * width : (d + 1) * width]
            served_ref[d, x] = out[(2 + d) * width : (3 + d) * width]


def flow_compute(weights, flow, received, s, start, rows, ahead, tokens):
    _, _, width, depth = flow.shape
    tile = min(rows, 4)
    block = pl.BlockSpec((tile, width, depth), lambda g: (g, 0, 0))

    def piece_of(s, start):
        return pl.BlockSpec((1, tile, width, depth), lambda g: (s, start // tile + g, 0, 0))

    n = weights.shape[1]
    later = [] if ahead is None else [ahead]
    return pl.pallas_call(
        functools.partial(flow_kernel, 1 + len(received), len(later)),
        grid=(rows // tile,),
        in_specs=[pl.BlockSpec(weights.shape, lambda g: (0, 0)), piece_of(s, start)]
        + [block] * len(received)
        + [piece_of(*at) for at in later]
        + [ANY_SPEC] * len(tokens),
        out_specs=[
            pl.BlockSpec((1, 2, tile, width, depth), lambda g: (0, 0, g, 0, 0)),
            pl.BlockSpec((2, tile, width, depth), lambda g: (0, g, 0, 0)),
        ]
        + [block] * len(later),
        out_shape=[
            jax.ShapeDtypeStruct((1, 2, rows, width, depth), jnp.bfloat16),
            jax.ShapeDtypeStruct((2, rows, width, depth), jnp.bfloat16),
        ]
        + [jax.ShapeDtypeStruct((rows, width, depth), jnp.bfloat16)] * len(later),
        compiler_params=params(),
        cost_estimate=cost(8 * rows * width * n * depth, 2 * rows * depth * (n + 4 * width)),
        name="flow_compute",
    )(weights, flow, *received, *[flow for _ in later], *tokens)


def pick_kernel(count, quarter, own_ref, got_ref, *refs):
    out_ref, token_ref = refs[-2:]
    me = lax.axis_index("col")
    inner = jnp.logical_and(me >= quarter, me < count - quarter)
    token_ref[...] = jnp.zeros_like(token_ref)

    @pl.when(inner)
    def _():
        out_ref[...] = own_ref[...]

    @pl.when(jnp.logical_not(inner))
    def _():
        out_ref[0] = got_ref[...]


def flow_pick(shape, own, got, whole, s, start, rows, count):
    tile = min(rows, 4)
    width, depth = shape[3:]
    operands = (own, got) + (() if whole is None else (whole,))
    return pl.pallas_call(
        functools.partial(pick_kernel, count, count // 4),
        grid=(rows // tile,),
        in_specs=[
            pl.BlockSpec((1, 2, tile, width, depth), lambda g: (0, 0, g, 0, 0)),
            pl.BlockSpec((2, tile, width, depth), lambda g: (0, g, 0, 0)),
        ]
        + [ANY_SPEC] * (len(operands) - 2),
        out_specs=[
            pl.BlockSpec(
                (1, 2, tile, width, depth), lambda g: (s, 0, start // tile + g, 0, 0)
            ),
            TOKEN_SPEC,
        ],
        out_shape=[jax.ShapeDtypeStruct(shape, jnp.bfloat16), TOKEN],
        input_output_aliases={2: 0} if whole is not None else {},
        compiler_params=params(),
        cost_estimate=cost(0, 12 * rows * width * depth),
        name="flow_pick",
    )(*operands)


def turn_kernel(in_ref, out_ref, scratch):
    _, width, tile, depth = in_ref.shape
    for h in range(depth // 128):
        part = in_ref[0, :, :, h * 128 : (h + 1) * 128].astype(jnp.float32)
        scratch[h] = part.reshape(width * tile, 128)
    for y in range(tile):
        for h in range(depth // 128):
            out_ref[y, :, h * 128 : (h + 1) * 128] = scratch[
                h, pl.ds(y, width, stride=tile), :
            ].astype(jnp.bfloat16)


def turn(species, s):
    _, width, rows, depth = species.shape
    tile = 16
    return pl.pallas_call(
        turn_kernel,
        grid=(rows // tile,),
        in_specs=[pl.BlockSpec((1, width, tile, depth), lambda g: (s, 0, g, 0))],
        out_specs=pl.BlockSpec((tile, width, depth), lambda g: (g, 0, 0)),
        out_shape=jax.ShapeDtypeStruct((rows, width, depth), jnp.bfloat16),
        scratch_shapes=[pltpu.VMEM((depth // 128, width * tile, 128), jnp.float32)],
        compiler_params=params(),
        cost_estimate=cost(0, 4 * rows * width * depth),
        name="turn",
    )(species)


def species_kernel(w_ref, lines_ref, *refs):
    out_ref, token_ref, scratch = refs[-3:]
    _, _, width, tile, depth = out_ref.shape
    token_ref[...] = jnp.zeros_like(token_ref)

    for y in range(tile):
        lines = jnp.concatenate([lines_ref[k, y] for k in range(lines_ref.shape[0])], axis=0)
        out = jnp.dot(w_ref[...], lines, preferred_element_type=jnp.float32)
        for h in range(depth // 128):
            scratch[h, pl.ds(y, 2 * width, stride=tile), :] = out[:, h * 128 : (h + 1) * 128]
    for h in range(depth // 128):
        for d in range(2):
            part = scratch[h, d * width * tile : (d + 1) * width * tile, :]
            out_ref[0, d, :, :, h * 128 : (h + 1) * 128] = part.reshape(
                width, tile, 128
            ).astype(jnp.bfloat16)


def species_compute(shape, weights, lines, whole, s, start, tokens):
    _, _, width, _, depth = shape
    count, rows = lines.shape[:2]
    tile = 16
    operands = (weights, lines) + (() if whole is None else (whole,)) + tuple(tokens)
    n = weights.shape[1]
    return pl.pallas_call(
        species_kernel,
        grid=(rows // tile,),
        in_specs=[
            pl.BlockSpec(weights.shape, lambda g: (0, 0)),
            pl.BlockSpec((count, tile, width, depth), lambda g: (0, g, 0, 0)),
        ]
        + [ANY_SPEC] * (len(operands) - 2),
        out_specs=[
            pl.BlockSpec(
                (1, 2, width, tile, depth), lambda g: (s, 0, 0, start // tile + g, 0)
            ),
            TOKEN_SPEC,
        ],
        out_shape=[jax.ShapeDtypeStruct(shape, jnp.bfloat16), TOKEN],
        scratch_shapes=[pltpu.VMEM((depth // 128, 2 * width * tile, 128), jnp.float32)],
        input_output_aliases={2: 0} if whole is not None else {},
        compiler_params=params(),
        cost_estimate=cost(4 * rows * width * n * depth, 2 * rows * depth * (n + 2 * width)),
        name="species_compute",
    )(*operands)


def operator_rows(operators, count, row, columns):
    width = operators.shape[1] // count
    rows = lax.dynamic_slice_in_dim(operators, row * width, width, axis=1)
    parts = [lax.dynamic_slice_in_dim(rows, c * width, width, axis=2) for c in columns]
    return jnp.concatenate(parts, axis=2).reshape(2 * width, count * width)


MESH = pl.DeviceIdType.MESH
ROWS = 1
WINDOW = 6
RING = 12
TURNED = 5
SERVED = 6
SENT = 8
BLOCK = 32
SLOTS = 8
NEAR = 2


def local(src, dst, sem):
    return pltpu.make_async_copy(src, dst, sem)


def remote(src, dst, sent, got, **to):
    return pltpu.make_async_remote_copy(src, dst, sent, got, device_id=to, device_id_type=MESH)


def exchange_kernel(
    rows_n, cols_n, x_ops, y_ops, species, flow, sp_far, sp_near, fl_out, gathered,
    weights, lines, own_v, served_o, t_in, t_out, g_v, sp_scratch, sp_o,
    weights_sem, lines_sem, sent_sem, credit, own_sem, served_sem, flow_sem,
    t_in_sem, t_out_sem, g_sem, g_v_sem, copy_sem, sp_o_sem, sp_sem,
):
    me, col = lax.axis_index("row"), lax.axis_index("col")
    kinds, width_x, width_y, depth = flow.shape
    partner, far, mirror = col + 1 - 2 * (col % 2), (col + 2) % 4, 3 - col
    inner = jnp.logical_and(col >= 1, col <= 2)
    outer = jnp.logical_not(inner)
    per = width_x // ROWS
    steps = kinds * per
    tile = width_y // rows_n
    units = kinds * rows_n
    first = 5 * steps // 16
    spread = steps - first - steps // 16

    @pl.when(inner)
    def _():
        for c, g in enumerate((col, partner, far, mirror)):
            for o, home in enumerate((col, partner)):
                for d in range(2):
                    block = y_ops.at[
                        d,
                        pl.ds(pl.multiple_of(home * width_y, width_y), width_y),
                        pl.ds(pl.multiple_of(g * width_y, width_y), width_y),
                    ]
                    at = pl.ds((2 * o + d) * width_y, width_y), pl.ds(c * width_y, width_y)
                    local(block, weights.at[at], weights_sem).start()

    barrier = pltpu.get_barrier_semaphore()
    for i in range(1, rows_n):
        pl.semaphore_signal(
            barrier, inc=1, device_id={"row": (me + i) % rows_n}, device_id_type=MESH
        )
    for i in range(1, cols_n):
        pl.semaphore_signal(
            barrier, inc=1, device_id={"col": (col + i) % cols_n}, device_id_type=MESH
        )
    pl.semaphore_wait(barrier, rows_n + cols_n - 2)

    def rows_of(ref, k):
        return ref.at[k // per, pl.ds((k % per) * ROWS, ROWS)]

    def pairs_of(ref, k):
        return ref.at[k // per, :, pl.ds((k % per) * ROWS, ROWS)]

    def piece(role, k, slot, to):
        at = lines.at[role, k % RING]
        return remote(
            rows_of(flow, k), at, sent_sem.at[min(role, 1), slot], lines_sem.at[role, k % RING],
            col=to,
        )

    def send(k):
        @pl.when(jnp.logical_and(outer, k >= RING))
        def _():
            pl.semaphore_wait(credit.at[0], 1)

        @pl.when(k >= RING)
        def _():
            pl.semaphore_wait(credit.at[1], 1)

        @pl.when(outer)
        def _():
            piece(0, k, k % WINDOW, partner).start()
            piece(1, k, k % WINDOW, far).start()

        @pl.when(inner)
        def _():
            piece(2, k, k % WINDOW, mirror).start()

    def sent(k):
        piece(1, k, k % WINDOW, far).wait_send()

        @pl.when(outer)
        def _():
            piece(0, k, k % WINDOW, partner).wait_send()

    def load_own(k):
        return local(rows_of(flow, k), own_v.at[k % 2], own_sem.at[k % 2])

    def serve(k):
        return remote(
            served_o.at[k % SERVED], pairs_of(fl_out, k), served_sem.at[k % SERVED],
            flow_sem.at[k // per], col=partner,
        )

    def load_turn(m):
        s, r = m // rows_n, (me + 1 + m % rows_n) % rows_n
        return local(species.at[s, :, pl.ds(r * tile, tile)], t_in.at[m % 2], t_in_sem.at[m % 2])

    def send_turn(m):
        s, r = m // rows_n, (me + 1 + m % rows_n) % rows_n
        return remote(
            t_out.at[m % TURNED], gathered.at[s, me], t_out_sem.at[m % TURNED], g_sem.at[s], row=r
        )

    def send_species(u, part=sp_far, s=0):
        r = (me + 1 + u % rows_n) % rows_n
        return remote(
            sp_o.at[u % SENT], part.at[s, :, :, pl.ds(me * tile, tile)],
            sp_o_sem.at[u % SENT], sp_sem.at[u // rows_n], row=r,
        )

    def away(m):
        return m % rows_n != rows_n - 1

    @pl.loop(0, WINDOW)
    def _(k):
        send(k)

    load_turn(0).start()

    @pl.when(inner)
    def _():
        load_own(0).start()
        local(y_ops.at[0], weights, weights_sem).wait()

    def turn_step(m):
        load_turn(m).wait()

        @pl.when(m + 1 < units)
        def _():
            load_turn(m + 1).start()

        @pl.when(jnp.logical_and(m >= TURNED, away(m - TURNED)))
        def _():
            send_turn(m - TURNED).wait_send()

        for h in range(depth // 128):
            part = t_in[m % 2, :, :, h * 128 : (h + 1) * 128].astype(jnp.float32)
            sp_scratch[h, : width_x * tile] = part.reshape(width_x * tile, 128)
        for y in range(tile):
            for h in range(depth // 128):
                t_out[m % TURNED, y, :, h * 128 : (h + 1) * 128] = sp_scratch[
                    h, pl.ds(y, width_x, stride=tile), :
                ].astype(jnp.bfloat16)

        @pl.when(away(m))
        def _():
            send_turn(m).start()

        @pl.when(jnp.logical_not(away(m)))
        def _():
            copy = local(t_out.at[m % TURNED], gathered.at[m // rows_n, me], copy_sem)
            copy.start()
            copy.wait()

    def load_species(s):
        return local(gathered.at[s], g_v, g_v_sem)

    def fetch_species(s):
        got = gathered.at[s, pl.ds(0, rows_n - 1)]
        remote(got, got, copy_sem, g_sem.at[s], row=me).wait_recv()
        load_species(s).start()

    def multiply(u, ys):
        r = (me + 1 + u % rows_n) % rows_n
        at = pl.ds(pl.multiple_of(r * width_x, width_x), width_x)
        for y in ys:
            block = jnp.concatenate([g_v[g, y] for g in range(rows_n)], axis=0)
            w = jnp.concatenate([x_ops[0, at], x_ops[1, at]], axis=0)
            out = jnp.dot(w, block, preferred_element_type=jnp.float32)
            for h in range(depth // 128):
                sp_scratch[h, pl.ds(y, 2 * width_x, stride=tile), :] = out[
                    :, h * 128 : (h + 1) * 128
                ]

    def begin_species(u):
        @pl.when(u % rows_n == 0)
        def _():
            load_species(u // rows_n).wait()

        multiply(u, range(tile // 2))

    def end_species(u):
        s = u // rows_n
        multiply(u, range(tile // 2, tile))

        @pl.when(u >= SENT)
        def _():
            send_species(u - SENT).wait_send()

        for h in range(depth // 128):
            for d in range(2):
                part = sp_scratch[h, d * width_x * tile : (d + 1) * width_x * tile, :]
                sp_o[u % SENT, d, :, :, h * 128 : (h + 1) * 128] = part.reshape(
                    width_x, tile, 128
                ).astype(jnp.bfloat16)

        for part, at, here in ((sp_near, s, s < NEAR), (sp_far, s - NEAR, s >= NEAR)):
            stay = part.at[at, :, :, pl.ds(me * tile, tile)]

            @pl.when(jnp.logical_and(away(u), here))
            def _():
                send_species(u, part, at).start()

            @pl.when(jnp.logical_and(jnp.logical_not(away(u)), here))
            def _():
                local(sp_o.at[u % SENT], stay, sp_o_sem.at[u % SENT]).start()

        @pl.when(jnp.logical_and(jnp.logical_not(away(u)), s + 1 < kinds))
        def _():
            fetch_species(s + 1)

    def flow_step(k):
        for role, source in enumerate((partner, far, mirror)):
            piece(role, k, k % WINDOW, source).wait_recv()
        load_own(k).wait()

        @pl.when(k + 1 < steps)
        def _():
            load_own(k + 1).start()

        @pl.when(k >= SERVED)
        def _():
            serve(k - SERVED).wait_send()

        for x in range(ROWS):
            block = jnp.concatenate(
                [own_v[k % 2, x]] + [lines[j, k % RING, x] for j in range(3)], axis=0
            )
            out = jnp.dot(weights[...], block, preferred_element_type=jnp.float32)
            out = out.astype(jnp.bfloat16)
            for d in range(2):
                served_o[k % SERVED, d, x] = out[(2 + d) * width_y : (3 + d) * width_y]
                fl_out[k // per, d, k % per * ROWS + x] = out[d * width_y : (d + 1) * width_y]
        serve(k).start()

        @pl.when(k + RING < steps)
        def _():
            for i, source in enumerate((partner, far, mirror)):
                pl.semaphore_signal(
                    credit.at[min(i, 1)], inc=1, device_id={"col": source}, device_id_type=MESH
                )

    @pl.loop(0, steps)
    def _(k):
        m = k * units // first

        @pl.when(jnp.logical_and(m < units, m != (k + 1) * units // first))
        def _():
            turn_step(m)

        @pl.when(k == first - 1)
        def _():
            fetch_species(0)

        past = (k - first) * 2 * units
        v = past // spread
        fresh = jnp.logical_and(k >= first, v != (past + 2 * units) // spread)

        @pl.when(jnp.logical_and(fresh, jnp.logical_and(v < 2 * units, v % 2 == 0)))
        def _():
            begin_species(v // 2)

        @pl.when(jnp.logical_and(fresh, jnp.logical_and(v < 2 * units, v % 2 == 1)))
        def _():
            end_species(v // 2)

        @pl.when(inner)
        def _():
            flow_step(k)

        sent(k)

        @pl.when(k + WINDOW < steps)
        def _():
            send(k + WINDOW)

    for m in range(units - TURNED, units):
        if m % rows_n != rows_n - 1:
            send_turn(m).wait_send()
    for u in range(units - SENT, units):
        send_species(u).wait_send()
    for s in range(kinds):
        part = sp_near.at[s] if s < NEAR else sp_far.at[s - NEAR]
        got = part.at[:, :, pl.ds(0, width_y - tile)]
        remote(got, got, copy_sem, sp_sem.at[s], row=me).wait_recv()

    @pl.when(inner)
    def _():
        for k in range(steps - SERVED, steps):
            serve(k).wait_send()

    @pl.when(outer)
    def _():
        for s in range(kinds):
            got = fl_out.at[s]
            remote(got, got, copy_sem, flow_sem.at[s], col=partner).wait_recv()


def settle_kernel(far, near, flow, sp_out, fl_out, held, in_sem, out_sem, near_sem):
    slots, rows = held.shape[:2]
    blocks, skip = far.shape[0] // rows, near.shape[0]

    def load(j):
        return local(far.at[pl.ds(j * rows, rows)], held.at[j % slots], in_sem.at[j % slots])

    def store(j):
        result = sp_out.at[pl.ds(skip + j * rows, rows)]
        return local(held.at[j % slots], result, out_sem.at[j % slots])

    ahead = slots // 2
    for j in range(min(ahead, blocks)):
        load(j).start()
    whole = [
        local(near, sp_out.at[pl.ds(0, skip)], near_sem.at[0]),
        local(flow, fl_out, near_sem.at[1]),
    ]
    for copy in whole:
        copy.start()
    for j in range(blocks):
        load(j).wait()
        store(j).start()
        if j + ahead < blocks:
            if j + ahead >= slots:
                store(j + ahead - slots).wait()
            load(j + ahead).start()
    for j in range(max(0, blocks - slots), blocks):
        store(j).wait()
    for copy in whole:
        copy.wait()


def settle(far, near, flow):
    shape = flow.shape
    far, near, flow = (a.reshape((-1,) + shape[3:]) for a in (far, near, flow))
    rows = min(far.shape[0], BLOCK)
    in_vmem = pl.BlockSpec(memory_space=pltpu.VMEM)
    results = pl.pallas_call(
        settle_kernel,
        in_specs=[ANY_SPEC, in_vmem, in_vmem],
        out_specs=[ANY_SPEC] * 2,
        out_shape=[jax.ShapeDtypeStruct(flow.shape, flow.dtype)] * 2,
        scratch_shapes=[
            pltpu.VMEM((SLOTS, rows) + shape[3:], jnp.bfloat16),
            pltpu.SemaphoreType.DMA((SLOTS,)),
            pltpu.SemaphoreType.DMA((SLOTS,)),
            pltpu.SemaphoreType.DMA((2,)),
        ],
        compiler_params=pltpu.CompilerParams(vmem_limit_bytes=20 * 1024 * 1024),
        cost_estimate=cost(0, 4 * far.size + 2 * near.size + 2 * flow.size),
        name="settle",
    )(far, *[pltpu.with_memory_space_constraint(a, pltpu.VMEM) for a in (near, flow)])
    return tuple(r.reshape(shape) for r in results)


def exchange(rows_n, cols_n, species, flow, x_operators, y_operators):
    kinds, width_x, width_y, depth = flow.shape
    tile = width_y // rows_n
    shape = (2, width_x, width_y, depth)
    kept = jax.ShapeDtypeStruct((kinds, rows_n, tile, width_x, depth), jnp.bfloat16)
    any_space = pl.BlockSpec(memory_space=pl.ANY)
    in_vmem = pl.BlockSpec(memory_space=pltpu.VMEM)
    dma = pltpu.SemaphoreType.DMA

    def vmem(*shape, dtype=jnp.bfloat16):
        return pltpu.VMEM(shape, dtype)

    halves = depth // 128
    far, near, flow_out, _ = pl.pallas_call(
        functools.partial(exchange_kernel, rows_n, cols_n),
        in_specs=[in_vmem, any_space, any_space, any_space],
        out_specs=[any_space, in_vmem, in_vmem, any_space],
        out_shape=[
            jax.ShapeDtypeStruct((kinds - NEAR,) + shape, jnp.bfloat16),
            pltpu.VMEM((NEAR,) + shape, jnp.bfloat16),
            pltpu.VMEM((kinds,) + shape, jnp.bfloat16),
            kept,
        ],
        scratch_shapes=[
            vmem(4 * width_y, cols_n * width_y),
            vmem(3, RING, ROWS, width_y, depth),
            vmem(2, ROWS, width_y, depth),
            vmem(SERVED, 2, ROWS, width_y, depth),
            vmem(2, width_x, tile, depth),
            vmem(TURNED, tile, width_x, depth),
            vmem(rows_n, tile, width_x, depth),
            vmem(halves, 2 * width_x * tile, 128, dtype=jnp.float32),
            vmem(SENT, 2, width_x, tile, depth),
            dma,
            dma((3, RING)),
            dma((2, WINDOW)),
            pltpu.SemaphoreType.REGULAR((2,)),
            dma((2,)),
            dma((SERVED,)),
            dma((kinds,)),
            dma((2,)),
            dma((TURNED,)),
            dma((kinds,)),
            dma,
            dma,
            dma((SENT,)),
            dma((kinds,)),
        ],
        compiler_params=pltpu.CompilerParams(
            collective_id=0, has_side_effects=True, vmem_limit_bytes=23 * 1024 * 1024 + 512 * 1024
        ),
        cost_estimate=cost(
            16 * kinds * width_x * width_y * cols_n * width_y * depth,
            12 * kinds * width_x * width_y * depth,
        ),
        name="exchange",
    )(x_operators, y_operators, species, flow)
    return settle(far, near, flow_out)


def body(rows_n, cols_n, species, flow, x_operators, y_operators):
    kinds, width_x, width_y, depth = species.shape
    out_shape = (kinds, 2, width_x, width_y, depth)
    if cols_n == 4 and width_y == 16 * rows_n and width_x % 16 == 0:
        return exchange(rows_n, cols_n, species, flow, x_operators, y_operators)

    quarter, half = cols_n // 4, cols_n // 2
    inner = [quarter + i for i in range(half)]
    outer = [i if i < quarter else i + half for i in range(half)]
    at = jnp.clip(lax.axis_index("col") - quarter, 0, half - 1)

    def inner_of(i):
        return quarter + i

    def outer_of(i):
        return jnp.where(i < quarter, i, i + half)

    plans, columns = [], [inner_of(at)]
    for k in range(half):
        plans.append([(outer[i], inner[(i + k) % half]) for i in range(half)])
        columns.append(outer_of((at - k) % half))
    for k in range(1, half):
        plans.append([(inner[i], inner[(i + k) % half]) for i in range(half)])
        columns.append(inner_of((at - k) % half))
    back = [(inner[i], outer[i]) for i in range(half)]
    y_weights = jnp.concatenate(
        [operator_rows(y_operators, cols_n, o, columns) for o in (inner_of(at), outer_of(at))]
    )

    row = lax.axis_index("row")
    x_weights = lax.dynamic_slice_in_dim(x_operators, row * width_x, width_x, axis=1)
    x_weights = x_weights.reshape(2 * width_x, rows_n * width_x)
    lines = [lax.all_gather(turn(species, s), "row") for s in range(kinds)]

    flow_rows = width_x // FLOW_SPLITS
    chunks = [(s, c * flow_rows) for s in range(kinds) for c in range(FLOW_SPLITS)]
    pieces = [flow[s, start : start + flow_rows] for s, start in chunks[:AHEAD]]
    received = [[lax.ppermute(piece, "col", plan) for plan in plans] for piece in pieces]

    when = {((s + 1) * len(chunks)) // kinds + LAG: s for s in range(kinds)}
    species_out, flow_out, results, order = None, None, [], []

    def multiply(s, after):
        return species_compute(out_shape, x_weights, lines[s], species_out, s, 0, after)

    def pick(k):
        s, start = chunks[k]
        return flow_pick(out_shape, *results[k], flow_out, s, start, flow_rows, cols_n)

    for k, (s, start) in enumerate(chunks):
        tokens = order
        if k in when:
            species_out, token = multiply(when[k], tokens)
            tokens = [token]
        ahead = chunks[k + AHEAD] if k + AHEAD < len(chunks) else None
        own, served, *piece = flow_compute(
            y_weights, flow, received[k], s, start, flow_rows, ahead, tokens
        )
        received.extend([lax.ppermute(p, "col", plan) for plan in plans] for p in piece)
        results.append((own, lax.ppermute(served, "col", back)))
        order = []
        if k >= BEHIND:
            flow_out, token = pick(k - BEHIND)
            order = [token]
    for k, s in when.items():
        if k >= len(chunks):
            species_out, token = multiply(s, order)
            order = [token]
    for k in range(len(chunks) - BEHIND, len(chunks)):
        flow_out, _ = pick(k)
    return (species_out, flow_out)


def solution(mesh):
    placed = (P(None, "row", "col", None), P(None, "row", "col", None), P(), P())
    return jax.shard_map(
        functools.partial(body, mesh.shape["row"], mesh.shape["col"]),
        mesh=mesh,
        in_specs=placed,
        out_specs=(P(None, None, "row", "col", None), P(None, None, "row", "col", None)),
        check_vma=False,
    )
```

```python
import functools

import jax
import jax.numpy as jnp
from jax import lax
from jax.experimental import pallas as pl
from jax.experimental.pallas import tpu as pltpu
from jax.sharding import PartitionSpec as P


FLOW_SPLITS = 4
AHEAD = 3
BEHIND = 3
LAG = 1
VMEM = 56 * 1024 * 1024


def params():
    return pltpu.CompilerParams(vmem_limit_bytes=VMEM)


def cost(flops, moved):
    return pl.CostEstimate(flops=flops, bytes_accessed=moved, transcendentals=0)


TOKEN = jax.ShapeDtypeStruct((8, 128), jnp.float32)
TOKEN_SPEC = pl.BlockSpec((8, 128), lambda g: (0, 0))
ANY_SPEC = pl.BlockSpec(memory_space=pl.ANY)


def flow_kernel(count, ahead, w_ref, *refs):
    sources, (own_ref, served_ref) = refs[:count], refs[-2 - ahead :][:2]
    width = own_ref.shape[3]
    if ahead:
        refs[-1][...] = refs[count][0]

    @pl.loop(0, own_ref.shape[2])
    def _(x):
        lines = jnp.concatenate(
            [s[0, x] if len(s.shape) == 4 else s[x] for s in sources], axis=0
        )
        out = jnp.dot(w_ref[...], lines, preferred_element_type=jnp.float32)
        out = out.astype(jnp.bfloat16)
        for d in range(2):
            own_ref[0, d, x] = out[d * width : (d + 1) * width]
            served_ref[d, x] = out[(2 + d) * width : (3 + d) * width]


def flow_compute(weights, flow, received, s, start, rows, ahead, tokens):
    _, _, width, depth = flow.shape
    tile = min(rows, 4)
    block = pl.BlockSpec((tile, width, depth), lambda g: (g, 0, 0))

    def piece_of(s, start):
        return pl.BlockSpec((1, tile, width, depth), lambda g: (s, start // tile + g, 0, 0))

    n = weights.shape[1]
    later = [] if ahead is None else [ahead]
    return pl.pallas_call(
        functools.partial(flow_kernel, 1 + len(received), len(later)),
        grid=(rows // tile,),
        in_specs=[pl.BlockSpec(weights.shape, lambda g: (0, 0)), piece_of(s, start)]
        + [block] * len(received)
        + [piece_of(*at) for at in later]
        + [ANY_SPEC] * len(tokens),
        out_specs=[
            pl.BlockSpec((1, 2, tile, width, depth), lambda g: (0, 0, g, 0, 0)),
            pl.BlockSpec((2, tile, width, depth), lambda g: (0, g, 0, 0)),
        ]
        + [block] * len(later),
        out_shape=[
            jax.ShapeDtypeStruct((1, 2, rows, width, depth), jnp.bfloat16),
            jax.ShapeDtypeStruct((2, rows, width, depth), jnp.bfloat16),
        ]
        + [jax.ShapeDtypeStruct((rows, width, depth), jnp.bfloat16)] * len(later),
        compiler_params=params(),
        cost_estimate=cost(8 * rows * width * n * depth, 2 * rows * depth * (n + 4 * width)),
        name="flow_compute",
    )(weights, flow, *received, *[flow for _ in later], *tokens)


def pick_kernel(count, quarter, own_ref, got_ref, *refs):
    out_ref, token_ref = refs[-2:]
    me = lax.axis_index("col")
    inner = jnp.logical_and(me >= quarter, me < count - quarter)
    token_ref[...] = jnp.zeros_like(token_ref)

    @pl.when(inner)
    def _():
        out_ref[...] = own_ref[...]

    @pl.when(jnp.logical_not(inner))
    def _():
        out_ref[0] = got_ref[...]


def flow_pick(shape, own, got, whole, s, start, rows, count):
    tile = min(rows, 4)
    width, depth = shape[3:]
    operands = (own, got) + (() if whole is None else (whole,))
    return pl.pallas_call(
        functools.partial(pick_kernel, count, count // 4),
        grid=(rows // tile,),
        in_specs=[
            pl.BlockSpec((1, 2, tile, width, depth), lambda g: (0, 0, g, 0, 0)),
            pl.BlockSpec((2, tile, width, depth), lambda g: (0, g, 0, 0)),
        ]
        + [ANY_SPEC] * (len(operands) - 2),
        out_specs=[
            pl.BlockSpec(
                (1, 2, tile, width, depth), lambda g: (s, 0, start // tile + g, 0, 0)
            ),
            TOKEN_SPEC,
        ],
        out_shape=[jax.ShapeDtypeStruct(shape, jnp.bfloat16), TOKEN],
        input_output_aliases={2: 0} if whole is not None else {},
        compiler_params=params(),
        cost_estimate=cost(0, 12 * rows * width * depth),
        name="flow_pick",
    )(*operands)


def turn_kernel(in_ref, out_ref, scratch):
    _, width, tile, depth = in_ref.shape
    for h in range(depth // 128):
        part = in_ref[0, :, :, h * 128 : (h + 1) * 128].astype(jnp.float32)
        scratch[h] = part.reshape(width * tile, 128)
    for y in range(tile):
        for h in range(depth // 128):
            out_ref[y, :, h * 128 : (h + 1) * 128] = scratch[
                h, pl.ds(y, width, stride=tile), :
            ].astype(jnp.bfloat16)


def turn(species, s):
    _, width, rows, depth = species.shape
    tile = 16
    return pl.pallas_call(
        turn_kernel,
        grid=(rows // tile,),
        in_specs=[pl.BlockSpec((1, width, tile, depth), lambda g: (s, 0, g, 0))],
        out_specs=pl.BlockSpec((tile, width, depth), lambda g: (g, 0, 0)),
        out_shape=jax.ShapeDtypeStruct((rows, width, depth), jnp.bfloat16),
        scratch_shapes=[pltpu.VMEM((depth // 128, width * tile, 128), jnp.float32)],
        compiler_params=params(),
        cost_estimate=cost(0, 4 * rows * width * depth),
        name="turn",
    )(species)


def species_kernel(w_ref, lines_ref, *refs):
    out_ref, token_ref, scratch = refs[-3:]
    _, _, width, tile, depth = out_ref.shape
    token_ref[...] = jnp.zeros_like(token_ref)

    for y in range(tile):
        lines = jnp.concatenate([lines_ref[k, y] for k in range(lines_ref.shape[0])], axis=0)
        out = jnp.dot(w_ref[...], lines, preferred_element_type=jnp.float32)
        for h in range(depth // 128):
            scratch[h, pl.ds(y, 2 * width, stride=tile), :] = out[:, h * 128 : (h + 1) * 128]
    for h in range(depth // 128):
        for d in range(2):
            part = scratch[h, d * width * tile : (d + 1) * width * tile, :]
            out_ref[0, d, :, :, h * 128 : (h + 1) * 128] = part.reshape(
                width, tile, 128
            ).astype(jnp.bfloat16)


def species_compute(shape, weights, lines, whole, s, start, tokens):
    _, _, width, _, depth = shape
    count, rows = lines.shape[:2]
    tile = 16
    operands = (weights, lines) + (() if whole is None else (whole,)) + tuple(tokens)
    n = weights.shape[1]
    return pl.pallas_call(
        species_kernel,
        grid=(rows // tile,),
        in_specs=[
            pl.BlockSpec(weights.shape, lambda g: (0, 0)),
            pl.BlockSpec((count, tile, width, depth), lambda g: (0, g, 0, 0)),
        ]
        + [ANY_SPEC] * (len(operands) - 2),
        out_specs=[
            pl.BlockSpec(
                (1, 2, width, tile, depth), lambda g: (s, 0, 0, start // tile + g, 0)
            ),
            TOKEN_SPEC,
        ],
        out_shape=[jax.ShapeDtypeStruct(shape, jnp.bfloat16), TOKEN],
        scratch_shapes=[pltpu.VMEM((depth // 128, 2 * width * tile, 128), jnp.float32)],
        input_output_aliases={2: 0} if whole is not None else {},
        compiler_params=params(),
        cost_estimate=cost(4 * rows * width * n * depth, 2 * rows * depth * (n + 2 * width)),
        name="species_compute",
    )(*operands)


def operator_rows(operators, count, row, columns):
    width = operators.shape[1] // count
    rows = lax.dynamic_slice_in_dim(operators, row * width, width, axis=1)
    parts = [lax.dynamic_slice_in_dim(rows, c * width, width, axis=2) for c in columns]
    return jnp.concatenate(parts, axis=2).reshape(2 * width, count * width)


MESH = pl.DeviceIdType.MESH
ROWS = 1
WINDOW = 5
RING = 10
TURNED = 4
SERVED = 4
SENT = 4
PIECE = 32
PARTS = 4


def local(src, dst, sem):
    return pltpu.make_async_copy(src, dst, sem)


def remote(src, dst, sent, got, **to):
    return pltpu.make_async_remote_copy(src, dst, sent, got, device_id=to, device_id_type=MESH)


def exchange_kernel(
    rows_n, cols_n, x_ops, y_ops, species, flow, sp_out, fl_out, gathered,
    weights, lines, own_v, served_o, t_in, t_out, g_v, sp_scratch, sp_o,
    weights_sem, lines_sem, sent_sem, credit, own_sem, served_sem, flow_sem,
    t_in_sem, t_out_sem, g_sem, g_v_sem, copy_sem, sp_o_sem, sp_sem,
):
    me, col = lax.axis_index("row"), lax.axis_index("col")
    kinds, width_x, width_y, depth = flow.shape
    partner, far, mirror = col + 1 - 2 * (col % 2), (col + 2) % 4, 3 - col
    inner = jnp.logical_and(col >= 1, col <= 2)
    outer = jnp.logical_not(inner)
    per = width_x // ROWS
    steps = kinds * per
    tile = width_y // rows_n
    units = kinds * rows_n
    first = 5 * steps // 16
    spread = steps - first - steps // 16

    @pl.when(inner)
    def _():
        for c, g in enumerate((col, partner, far, mirror)):
            for o, home in enumerate((col, partner)):
                for d in range(2):
                    block = y_ops.at[
                        d,
                        pl.ds(pl.multiple_of(home * width_y, width_y), width_y),
                        pl.ds(pl.multiple_of(g * width_y, width_y), width_y),
                    ]
                    at = pl.ds((2 * o + d) * width_y, width_y), pl.ds(c * width_y, width_y)
                    local(block, weights.at[at], weights_sem).start()

    barrier = pltpu.get_barrier_semaphore()
    for i in range(1, rows_n):
        pl.semaphore_signal(
            barrier, inc=1, device_id={"row": (me + i) % rows_n}, device_id_type=MESH
        )
    for i in range(1, cols_n):
        pl.semaphore_signal(
            barrier, inc=1, device_id={"col": (col + i) % cols_n}, device_id_type=MESH
        )
    pl.semaphore_wait(barrier, rows_n + cols_n - 2)

    def target(i):
        late, step, back = i // 4, i + me % 2, (7 - i) // 2
        dx = (1 - late) * ((step + 1) % 2) + late * back
        dy = (1 - late) * (step % 2) + late * back
        dc = (1 - late) * (i // 2) + late * ((i + 1) // 2 % 2)
        return (me // 4 + dy) % 2 * 4 + (me // 2 + dx) % 2 * 2 + (me + dc) % 2

    def rows_of(ref, k):
        return ref.at[k // per, pl.ds((k % per) * ROWS, ROWS)]

    def pairs_of(ref, k):
        return ref.at[k // per, :, pl.ds((k % per) * ROWS, ROWS)]

    def piece(role, k, slot, to):
        at = lines.at[role, k % RING]
        return remote(
            rows_of(flow, k), at, sent_sem.at[min(role, 1), slot], lines_sem.at[role, k % RING],
            col=to,
        )

    def send(k):
        @pl.when(jnp.logical_and(outer, k >= RING))
        def _():
            pl.semaphore_wait(credit.at[0], 1)

        @pl.when(k >= RING)
        def _():
            pl.semaphore_wait(credit.at[1], 1)

        @pl.when(outer)
        def _():
            piece(1, k, k % WINDOW, far).start()
            piece(0, k, k % WINDOW, partner).start()

        @pl.when(inner)
        def _():
            piece(2, k, k % WINDOW, mirror).start()

    def sent(k):
        piece(1, k, k % WINDOW, far).wait_send()

        @pl.when(outer)
        def _():
            piece(0, k, k % WINDOW, partner).wait_send()

    def load_own(k):
        return local(rows_of(flow, k), own_v.at[k % 2], own_sem.at[k % 2])

    def serve(k):
        return remote(
            served_o.at[k % SERVED], pairs_of(fl_out, k), served_sem.at[k % SERVED],
            flow_sem.at[k // per], col=partner,
        )

    def load_turn(m):
        s, r = m // rows_n, target(m % rows_n)
        return local(species.at[s, :, pl.ds(r * tile, tile)], t_in.at[m % 2], t_in_sem.at[m % 2])

    def send_turn(m):
        s, r = m // rows_n, target(m % rows_n)
        return remote(
            t_out.at[m % TURNED], gathered.at[s, me], t_out_sem.at[m % TURNED], g_sem.at[s], row=r
        )

    def send_species(u):
        s, r = u // rows_n, target(u % rows_n)
        return remote(
            sp_o.at[u % SENT], sp_out.at[s, :, :, pl.ds(me * tile, tile)],
            sp_o_sem.at[u % SENT], sp_sem.at[s], row=r,
        )

    def away(m):
        return m % rows_n != rows_n - 1

    @pl.loop(0, WINDOW)
    def _(k):
        send(k)

    load_turn(0).start()

    @pl.when(inner)
    def _():
        load_own(0).start()
        local(y_ops.at[0], weights, weights_sem).wait()

    def turn_step(m):
        load_turn(m).wait()

        @pl.when(m + 1 < units)
        def _():
            load_turn(m + 1).start()

        @pl.when(jnp.logical_and(m >= TURNED, away(m - TURNED)))
        def _():
            send_turn(m - TURNED).wait_send()

        for h in range(depth // 128):
            part = t_in[m % 2, :, :, h * 128 : (h + 1) * 128].astype(jnp.float32)
            sp_scratch[h, : width_x * tile] = part.reshape(width_x * tile, 128)
        for y in range(tile):
            for h in range(depth // 128):
                t_out[m % TURNED, y, :, h * 128 : (h + 1) * 128] = sp_scratch[
                    h, pl.ds(y, width_x, stride=tile), :
                ].astype(jnp.bfloat16)

        @pl.when(away(m))
        def _():
            send_turn(m).start()

        @pl.when(jnp.logical_not(away(m)))
        def _():
            copy = local(t_out.at[m % TURNED], gathered.at[m // rows_n, me], copy_sem)
            copy.start()
            copy.wait()

    def load_part(q):
        at = pl.ds(q % PARTS * (tile // PARTS), tile // PARTS)
        return local(
            gathered.at[q // (PARTS * rows_n), :, at], g_v.at[q % 2], g_v_sem.at[q % 2]
        )

    def fetch_part(q):
        s = q // (PARTS * rows_n)

        @pl.when(q % (PARTS * rows_n) == 0)
        def _():
            got = gathered.at[s, pl.ds(0, rows_n - 1)]
            remote(got, got, copy_sem, g_sem.at[s], row=me).wait_recv()

        load_part(q).start()

    def part_of_species(u, p):
        q = u * PARTS + p
        load_part(q).wait()

        @pl.when(q + 1 < PARTS * units)
        def _():
            fetch_part(q + 1)

        r = target(u % rows_n)
        at = pl.ds(pl.multiple_of(r * width_x, width_x), width_x)
        for y in range(tile // PARTS):
            block = jnp.concatenate([g_v[q % 2, g, y] for g in range(rows_n)], axis=0)
            w = jnp.concatenate([x_ops[0, at], x_ops[1, at]], axis=0)
            out = jnp.dot(w, block, preferred_element_type=jnp.float32)
            row = p * (tile // PARTS) + y
            for h in range(depth // 128):
                sp_scratch[h, pl.ds(row, 2 * width_x, stride=tile), :] = out[
                    :, h * 128 : (h + 1) * 128
                ]

    def end_species(u):
        @pl.when(jnp.logical_and(u >= SENT, away(u - SENT)))
        def _():
            send_species(u - SENT).wait_send()

        for h in range(depth // 128):
            for d in range(2):
                part = sp_scratch[h, d * width_x * tile : (d + 1) * width_x * tile, :]
                sp_o[u % SENT, d, :, :, h * 128 : (h + 1) * 128] = part.reshape(
                    width_x, tile, 128
                ).astype(jnp.bfloat16)

        @pl.when(away(u))
        def _():
            send_species(u).start()

        @pl.when(jnp.logical_not(away(u)))
        def _():
            stay = sp_out.at[u // rows_n, :, :, pl.ds(me * tile, tile)]
            for d in range(2):
                stay[d] = sp_o[u % SENT, d]

    def flow_step(k):
        for role, source in enumerate((partner, far, mirror)):
            piece(role, k, k % WINDOW, source).wait_recv()
        load_own(k).wait()

        @pl.when(k + 1 < steps)
        def _():
            load_own(k + 1).start()

        @pl.when(k >= SERVED)
        def _():
            serve(k - SERVED).wait_send()

        for x in range(ROWS):
            block = jnp.concatenate(
                [own_v[k % 2, x]] + [lines[j, k % RING, x] for j in range(3)], axis=0
            )
            out = jnp.dot(weights[...], block, preferred_element_type=jnp.float32)
            out = out.astype(jnp.bfloat16)
            for d in range(2):
                served_o[k % SERVED, d, x] = out[(2 + d) * width_y : (3 + d) * width_y]
                fl_out[k // per, d, k % per * ROWS + x] = out[d * width_y : (d + 1) * width_y]
        serve(k).start()

        @pl.when(k + RING < steps)
        def _():
            for i, source in enumerate((partner, far, mirror)):
                pl.semaphore_signal(
                    credit.at[min(i, 1)], inc=1, device_id={"col": source}, device_id_type=MESH
                )

    @pl.loop(0, steps)
    def _(k):
        m = k * units // first

        @pl.when(jnp.logical_and(m < units, m != (k + 1) * units // first))
        def _():
            turn_step(m)

        @pl.when(k == first - 1)
        def _():
            fetch_part(0)

        each = PARTS + 1
        past = (k - first) * each * units
        v = past // spread
        fresh = jnp.logical_and(k >= first, v != (past + each * units) // spread)
        fresh = jnp.logical_and(fresh, v < each * units)
        for p in range(PARTS):

            @pl.when(jnp.logical_and(fresh, v % each == p))
            def _():
                part_of_species(v // each, p)

        @pl.when(jnp.logical_and(fresh, v % each == PARTS))
        def _():
            end_species(v // each)

        @pl.when(inner)
        def _():
            flow_step(k)

        sent(k)

        @pl.when(k + WINDOW < steps)
        def _():
            send(k + WINDOW)

    for m in range(units - TURNED, units):
        if m % rows_n != rows_n - 1:
            send_turn(m).wait_send()
    for u in range(units - SENT, units):
        if u % rows_n != rows_n - 1:
            send_species(u).wait_send()
    for s in range(kinds):
        got = sp_out.at[s, :, :, pl.ds(0, width_y - tile)]
        remote(got, got, copy_sem, sp_sem.at[s], row=me).wait_recv()

    @pl.when(inner)
    def _():
        for k in range(steps - SERVED, steps):
            serve(k).wait_send()

    @pl.when(outer)
    def _():
        for s in range(kinds):
            got = fl_out.at[s]
            remote(got, got, copy_sem, flow_sem.at[s], col=partner).wait_recv()


def settle_kernel(count, *refs):
    sems = refs[-1]
    copies = []
    for source, result in zip(refs[:count], refs[count : 2 * count]):
        for start in range(0, source.shape[0], PIECE):
            at = pl.ds(start, min(PIECE, source.shape[0] - start))
            copies.append(local(source.at[at], result.at[at], sems.at[len(copies)]))
    for copy in copies:
        copy.start()
    for copy in copies:
        copy.wait()


def settle(*held):
    flat = [a.reshape((-1,) + a.shape[3:]) for a in held]
    results = pl.pallas_call(
        functools.partial(settle_kernel, len(flat)),
        in_specs=[pl.BlockSpec(memory_space=pltpu.VMEM)] * len(flat),
        out_specs=[ANY_SPEC] * len(flat),
        out_shape=[jax.ShapeDtypeStruct(a.shape, a.dtype) for a in flat],
        scratch_shapes=[
            pltpu.SemaphoreType.DMA((sum(-(-a.shape[0] // PIECE) for a in flat),)),
        ],
        compiler_params=pltpu.CompilerParams(vmem_limit_bytes=(15 * 1024 + 900) * 1024),
        cost_estimate=cost(0, sum(2 * a.size for a in flat)),
        name="settle",
    )(*[pltpu.with_memory_space_constraint(a, pltpu.VMEM) for a in flat])
    return tuple(r.reshape(a.shape) for r, a in zip(results, held))


def exchange(rows_n, cols_n, species, flow, x_operators, y_operators):
    kinds, width_x, width_y, depth = flow.shape
    tile = width_y // rows_n
    shape = (2, width_x, width_y, depth)
    kept = jax.ShapeDtypeStruct((kinds, rows_n, tile, width_x, depth), jnp.bfloat16)
    any_space = pl.BlockSpec(memory_space=pl.ANY)
    in_vmem = pl.BlockSpec(memory_space=pltpu.VMEM)
    dma = pltpu.SemaphoreType.DMA

    def vmem(*shape, dtype=jnp.bfloat16):
        return pltpu.VMEM(shape, dtype)

    halves = depth // 128
    species_out, flow_out, _ = pl.pallas_call(
        functools.partial(exchange_kernel, rows_n, cols_n),
        in_specs=[in_vmem, any_space, any_space, any_space],
        out_specs=[in_vmem, in_vmem, any_space],
        out_shape=[
            pltpu.VMEM((kinds,) + shape, jnp.bfloat16),
            pltpu.VMEM((kinds,) + shape, jnp.bfloat16),
            kept,
        ],
        scratch_shapes=[
            vmem(4 * width_y, cols_n * width_y),
            vmem(3, RING, ROWS, width_y, depth),
            vmem(2, ROWS, width_y, depth),
            vmem(SERVED, 2, ROWS, width_y, depth),
            vmem(2, width_x, tile, depth),
            vmem(TURNED, tile, width_x, depth),
            vmem(2, rows_n, tile // PARTS, width_x, depth),
            vmem(halves, 2 * width_x * tile, 128, dtype=jnp.float32),
            vmem(SENT, 2, width_x, tile, depth),
            dma,
            dma((3, RING)),
            dma((2, WINDOW)),
            pltpu.SemaphoreType.REGULAR((2,)),
            dma((2,)),
            dma((SERVED,)),
            dma((kinds,)),
            dma((2,)),
            dma((TURNED,)),
            dma((kinds,)),
            dma((2,)),
            dma,
            dma((SENT,)),
            dma((kinds,)),
        ],
        compiler_params=pltpu.CompilerParams(
            collective_id=0, has_side_effects=True, vmem_limit_bytes=(15 * 1024 + 900) * 1024
        ),
        cost_estimate=cost(
            16 * kinds * width_x * width_y * cols_n * width_y * depth,
            12 * kinds * width_x * width_y * depth,
        ),
        name="exchange",
    )(x_operators, y_operators, species, flow)
    return settle(species_out, flow_out)


def body(rows_n, cols_n, species, flow, x_operators, y_operators):
    kinds, width_x, width_y, depth = species.shape
    out_shape = (kinds, 2, width_x, width_y, depth)
    if cols_n == 4 and rows_n == 8 and width_y == 16 * rows_n and width_x >= 8 * rows_n:
        return exchange(rows_n, cols_n, species, flow, x_operators, y_operators)

    quarter, half = cols_n // 4, cols_n // 2
    inner = [quarter + i for i in range(half)]
    outer = [i if i < quarter else i + half for i in range(half)]
    at = jnp.clip(lax.axis_index("col") - quarter, 0, half - 1)

    def inner_of(i):
        return quarter + i

    def outer_of(i):
        return jnp.where(i < quarter, i, i + half)

    plans, columns = [], [inner_of(at)]
    for k in range(half):
        plans.append([(outer[i], inner[(i + k) % half]) for i in range(half)])
        columns.append(outer_of((at - k) % half))
    for k in range(1, half):
        plans.append([(inner[i], inner[(i + k) % half]) for i in range(half)])
        columns.append(inner_of((at - k) % half))
    back = [(inner[i], outer[i]) for i in range(half)]
    y_weights = jnp.concatenate(
        [operator_rows(y_operators, cols_n, o, columns) for o in (inner_of(at), outer_of(at))]
    )

    row = lax.axis_index("row")
    x_weights = lax.dynamic_slice_in_dim(x_operators, row * width_x, width_x, axis=1)
    x_weights = x_weights.reshape(2 * width_x, rows_n * width_x)
    lines = [lax.all_gather(turn(species, s), "row") for s in range(kinds)]

    flow_rows = width_x // FLOW_SPLITS
    chunks = [(s, c * flow_rows) for s in range(kinds) for c in range(FLOW_SPLITS)]
    pieces = [flow[s, start : start + flow_rows] for s, start in chunks[:AHEAD]]
    received = [[lax.ppermute(piece, "col", plan) for plan in plans] for piece in pieces]

    when = {((s + 1) * len(chunks)) // kinds + LAG: s for s in range(kinds)}
    species_out, flow_out, results, order = None, None, [], []

    def multiply(s, after):
        return species_compute(out_shape, x_weights, lines[s], species_out, s, 0, after)

    def pick(k):
        s, start = chunks[k]
        return flow_pick(out_shape, *results[k], flow_out, s, start, flow_rows, cols_n)

    for k, (s, start) in enumerate(chunks):
        tokens = order
        if k in when:
            species_out, token = multiply(when[k], tokens)
            tokens = [token]
        ahead = chunks[k + AHEAD] if k + AHEAD < len(chunks) else None
        own, served, *piece = flow_compute(
            y_weights, flow, received[k], s, start, flow_rows, ahead, tokens
        )
        received.extend([lax.ppermute(p, "col", plan) for plan in plans] for p in piece)
        results.append((own, lax.ppermute(served, "col", back)))
        order = []
        if k >= BEHIND:
            flow_out, token = pick(k - BEHIND)
            order = [token]
    for k, s in when.items():
        if k >= len(chunks):
            species_out, token = multiply(s, order)
            order = [token]
    for k in range(len(chunks) - BEHIND, len(chunks)):
        flow_out, _ = pick(k)
    return (species_out, flow_out)


def solution(mesh):
    placed = (P(None, "row", "col", None), P(None, "row", "col", None), P(), P())
    return jax.shard_map(
        functools.partial(body, mesh.shape["row"], mesh.shape["col"]),
        mesh=mesh,
        in_specs=placed,
        out_specs=(P(None, None, "row", "col", None), P(None, None, "row", "col", None)),
        check_vma=False,
    )
```
